8 devices in a mesh: dp: 1 (over z), sp: 8 (over y, x, core).
Axes of the slice: x: 2, y: 2, z: 1, core: 2. Of those that a mesh axis runs over, the one named last changes fastest.
Arguments:
- z_points: bfloat16 [4096, 128], P(('dp', 'sp'))
- x_points: bfloat16 [65536, 128], P(('dp', 'sp'))
- rhs_vals: bfloat16 [65536, 16], P(('dp', 'sp'))
- block_mask: int32 [8, 8], P(('dp', 'sp'))
- length_scale: float32 [1], replicated
- out_scale: float32 [1], replicated
Outputs:
- output: float32 [4096, 16], P(('dp', 'sp'))
All inputs are finite; a program needn't handle non-finite values.
Results may differ from the reference program's by a relative error of at most 0.001.
Values are sent between devices in bfloat16 or wider.
A program may use at most 1 GiB of HBM per device.

```python
import jax
import jax.numpy as jnp
from jax import lax

D = 128
R = 16
SP = 8
TGT_DEV = 512
SRC_DEV = 8192
CLUSTERS = 8
M_TGT = SP * TGT_DEV
N_SRC = SP * SRC_DEV


def draw_mask(mask_key):
    key_a, key_b = jax.random.split(mask_key)
    mask_draws = jax.random.randint(key_a, (SP, SP), 0, SP)
    limits = jax.random.randint(key_b, (SP, 1), 1, SP + 1)
    on_diag = jnp.arange(SP)[:, None] == jnp.arange(SP)[None, :]
    return jnp.where((mask_draws < limits) | on_diag, 1, 0).astype(jnp.int32)


def setup_inputs(seed: int = 0, part: int = 0) -> dict:
    base_key = jax.random.key(seed)
    shared_key, part_base = jax.random.split(base_key)
    part_key = jax.random.fold_in(part_base, part)
    key_list = jax.random.split(part_key, 9)
    centers = jax.random.normal(key_list[0], (CLUSTERS, D), jnp.float32)
    z_labels = jax.random.randint(key_list[1], (M_TGT,), 0, CLUSTERS)
    x_labels = jax.random.randint(key_list[2], (N_SRC,), 0, CLUSTERS)
    z_vals = centers[z_labels] + 0.5 * jax.random.normal(key_list[3], (M_TGT, D), jnp.float32)
    x_vals = centers[x_labels] + 0.5 * jax.random.normal(key_list[4], (N_SRC, D), jnp.float32)
    col_mean = jax.random.uniform(key_list[5], (1, R), jnp.float32, minval=0.5, maxval=1.5)
    cluster_offs = jax.random.normal(key_list[6], (CLUSTERS, R), jnp.float32)
    rhs_noise = jax.random.normal(key_list[7], (N_SRC, R), jnp.float32)
    rhs = (col_mean + cluster_offs[x_labels] + rhs_noise) * (4.0 / N_SRC)
    block_mask = draw_mask(key_list[8])
    scale_keys = jax.random.split(shared_key)
    length_scale = jnp.sqrt(D * jax.random.uniform(scale_keys[0], (1,), jnp.float32, minval=0.8, maxval=1.4))
    out_scale = jax.random.uniform(scale_keys[1], (1,), jnp.float32, minval=0.5, maxval=1.5)
    return {
        "z_points": z_vals.astype(jnp.bfloat16),
        "x_points": x_vals.astype(jnp.bfloat16),
        "rhs_vals": rhs.astype(jnp.bfloat16),
        "block_mask": block_mask,
        "length_scale": length_scale,
        "out_scale": out_scale,
    }


def reference(z_points, x_points, rhs_vals, block_mask, length_scale, out_scale):
    ell_sq = length_scale[0] * length_scale[0]
    x_f32 = x_points.astype(jnp.float32)
    x_norm = jnp.sum(x_f32 * x_f32, axis=1)
    v_blocks = rhs_vals.reshape(SP, SRC_DEV, R)
    z_blocks = z_points.reshape(SP, TGT_DEV, D)

    def one_block(block_in):
        z_rows, mask_row = block_in
        z_f32 = z_rows.astype(jnp.float32)
        z_norm = jnp.sum(z_f32 * z_f32, axis=1)
        gram_mat = jnp.dot(z_rows, x_points.T, preferred_element_type=jnp.float32)
        sq_dist = jnp.maximum(z_norm[:, None] + x_norm[None, :] - 2.0 * gram_mat, 0.0)
        kern_mat = (out_scale[0] * jnp.exp(-sq_dist / (2.0 * ell_sq))).astype(jnp.bfloat16)
        v_masked = (v_blocks * mask_row[:, None, None].astype(jnp.bfloat16)).reshape(N_SRC, R)
        return jnp.dot(kern_mat, v_masked, preferred_element_type=jnp.float32)

    y_blocks = lax.map(one_block, (z_blocks, block_mask))
    return y_blocks.reshape(M_TGT, R)
```

```python
import jax
import jax.numpy as jnp
from jax import lax
from jax.experimental import pallas as pl
from jax.experimental.pallas import tpu as pltpu
from jax.sharding import PartitionSpec as P

F32 = jnp.float32
BF16 = jnp.bfloat16
LOG2E = 1.4426950408889634
TILE = 256
CHUNK = 2048
ZROWS = 144
ORDER = (1, 2, 4, 3, 5, 6, 7)


def limbs(r):
    first = r.astype(BF16).astype(F32)
    rest = jnp.where(jnp.abs(first) < jnp.inf, r - first, 0.0)
    second = rest.astype(BF16).astype(F32)
    return first, second, rest - second


def kernel(ls_ref, os_ref, w_ref, z_hbm, x_hbm, v_hbm, o_ref,
           zin, xs, vs, xaug, zall, ysend, yrecv, own,
           in_sem, zs_sem, zr_sem, ys_sem, yr_sem):
    me = lax.axis_index("sp")
    dp = lax.axis_index("dp")
    my_core, my_x, my_y = me % 2, (me // 2) % 2, me // 4

    def peer(k):
        c = (my_core + k % 2) % 2
        x = (my_x + (k // 2) % 2) % 2
        y = (my_y + k // 4) % 2
        return (y * 2 + x) * 2 + c

    zcopy = pltpu.make_async_copy(z_hbm, zin, in_sem.at[0])
    xcopy = pltpu.make_async_copy(x_hbm, xs, in_sem.at[1])
    vcopy = pltpu.make_async_copy(v_hbm, vs, in_sem.at[2])
    zcopy.start()
    xcopy.start()
    vcopy.start()
    barrier = pltpu.get_barrier_semaphore()
    for k in range(1, 8):
        pl.semaphore_signal(barrier, inc=1, device_id=(dp, peer(k)), device_id_type=pl.DeviceIdType.MESH)

    lv = jnp.full((8, 128), ls_ref[0], F32)
    l2 = lv * lv
    pv = jnp.where(l2 > 2.0**64, 2.0**-64, 1.0)
    l2p = l2 * pv
    cvec = LOG2E / l2p
    lns = l2p * jnp.log(jnp.full((8, 128), os_ref[0], F32))
    c = cvec[0, 0]
    s = os_ref[0].astype(BF16)
    sub = lax.broadcasted_iota(jnp.int32, (16, 128), 0)

    zcopy.wait()
    for q in range(4):
        zt = zin[pl.ds(128 * q, 128), :].astype(F32).T
        nz = jnp.sum(zt * zt, axis=0, keepdims=True)
        r = jnp.broadcast_to(nz, (16, 128)) * (-0.5 * pv[0:1, :]) + lns[0:1, :]
        a, b, d = limbs(r)
        aug = jnp.where(sub < 3, 1.0, jnp.where(sub == 3, a, jnp.where(sub == 4, b, jnp.where(sub == 5, d, 0.0))))
        zall[0, q, 0:128, :] = (zt * pv[0:1, :]).astype(BF16)
        zall[0, q, 128:144, :] = aug.astype(BF16)

    def zsend(k):
        return pltpu.make_async_remote_copy(
            src_ref=zall.at[0], dst_ref=zall.at[k], send_sem=zs_sem.at[k - 1], recv_sem=zr_sem.at[k - 1],
            device_id=(dp, peer(k)), device_id_type=pl.DeviceIdType.MESH)

    def ycopy(k):
        return pltpu.make_async_remote_copy(
            src_ref=ysend.at[k - 1], dst_ref=yrecv.at[k - 1], send_sem=ys_sem.at[k - 1], recv_sem=yr_sem.at[k - 1],
            device_id=(dp, peer(k)), device_id_type=pl.DeviceIdType.MESH)

    n_src = xs.shape[0]
    lane = lax.broadcasted_iota(jnp.int32, (TILE, 128), 1)

    def prep(i, carry):
        r0 = pl.multiple_of(i * TILE, TILE)
        xf = xs[pl.ds(r0, TILE), :].astype(F32)
        nx = jnp.sum(xf * xf, axis=1, keepdims=True)
        r = jnp.broadcast_to(nx, (TILE, 128)) * (-0.5 * pv[0:1, :])
        a, b, d = limbs(r)
        aug = jnp.where(lane == 0, a, jnp.where(lane == 1, b, jnp.where(lane == 2, d, jnp.where(lane < 6, 1.0, 0.0))))
        xaug[pl.ds(r0, TILE), :] = aug.astype(BF16)
        return carry

    zero_rows = jnp.zeros((256 - ZROWS, 512), BF16)

    def segment(slot, r0, r1):
        rhs = jnp.concatenate([zall[slot, q] for q in range(4)], axis=1)
        rhs = jnp.concatenate([rhs, zero_rows], axis=0)

        def chunk(i, acc):
            at = pl.multiple_of(i * CHUNK, CHUNK)
            lhs = jnp.concatenate([xs[pl.ds(at, CHUNK), :], xaug[pl.ds(at, CHUNK), :]], axis=1)
            t = jnp.dot(lhs, rhs, preferred_element_type=F32)
            kern = jnp.minimum(jnp.exp2(t * c).astype(BF16), s)
            return acc + jnp.dot(vs[:, pl.ds(at, CHUNK)], kern, preferred_element_type=F32)

        return lax.fori_loop(r0 // CHUNK, r1 // CHUNK, chunk, jnp.zeros((16, 512), F32))

    half = n_src // 2
    xcopy.wait()
    lax.fori_loop(0, half // TILE, prep, 0)
    pl.semaphore_wait(barrier, 7)
    for k in ORDER:
        zsend(k).start()
    lax.fori_loop(half // TILE, n_src // TILE, prep, 0)
    vcopy.wait()
    own[...] = segment(0, 0, half)

    def one(i, table):
        k = table % 8
        zsend(k).wait_recv()
        ysend[k - 1] = segment(k, 0, n_src)
        ycopy(k).start()
        return table // 8

    lax.fori_loop(0, 7, one, sum(k * 8**i for i, k in enumerate(ORDER)))
    own[...] += segment(0, half, n_src)
    total = own[...] * w_ref[0, me].astype(F32)
    for k in ORDER:
        ycopy(k).wait_recv()
        total = total + yrecv[k - 1] * w_ref[0, peer(k)].astype(F32)
    o_ref[...] = total
    for k in ORDER:
        zsend(k).wait_send()
        ycopy(k).wait_send()


def solution(mesh):
    row_spec = P(("dp", "sp"), None)

    def local_fn(z_rows, x_rows, v_rows, mask_row, length_scale, out_scale):
        n_src, r_cols = v_rows.shape
        n_tgt, depth = z_rows.shape
        smem = pl.BlockSpec(memory_space=pltpu.SMEM)
        anywhere = pl.BlockSpec(memory_space=pl.ANY)
        y_t = pl.pallas_call(
            kernel,
            out_shape=jax.ShapeDtypeStruct((r_cols, n_tgt), F32),
            in_specs=[smem, smem, smem, anywhere, anywhere, anywhere],
            out_specs=pl.BlockSpec(memory_space=pltpu.VMEM),
            scratch_shapes=[
                pltpu.VMEM((n_tgt, depth), BF16),
                pltpu.VMEM((n_src, depth), BF16),
                pltpu.VMEM((r_cols, n_src), BF16),
                pltpu.VMEM((n_src, 128), BF16),
                pltpu.VMEM((8, 4, ZROWS, 128), BF16),
                pltpu.VMEM((7, r_cols, n_tgt), F32),
                pltpu.VMEM((7, r_cols, n_tgt), F32),
                pltpu.VMEM((r_cols, n_tgt), F32),
                pltpu.SemaphoreType.DMA((3,)),
                pltpu.SemaphoreType.DMA((7,)),
                pltpu.SemaphoreType.DMA((7,)),
                pltpu.SemaphoreType.DMA((7,)),
                pltpu.SemaphoreType.DMA((7,)),
            ],
            compiler_params=pltpu.CompilerParams(
                collective_id=0, has_side_effects=True, vmem_limit_bytes=40 * 2**20),
        )(length_scale, out_scale, mask_row, z_rows, x_rows, v_rows.T)
        return y_t.T

    return jax.shard_map(local_fn, mesh=mesh, in_specs=(row_spec, row_spec, row_spec, row_spec, P(None), P(None)),
                         out_specs=row_spec, check_vma=False)
```

```python
import jax
import jax.numpy as jnp
from jax import lax
from jax.experimental import pallas as pl
from jax.experimental.pallas import tpu as pltpu
from jax.sharding import PartitionSpec as P

F32 = jnp.float32
BF16 = jnp.bfloat16
LOG2E = 1.4426950408889634
TILE = 256
CHUNK = 4096
ZROWS = 144
ORDER = (1, 2, 4, 3, 5, 6, 7)


def limbs(r):
    first = r.astype(BF16).astype(F32)
    rest = jnp.where(jnp.abs(first) < jnp.inf, r - first, 0.0)
    second = rest.astype(BF16).astype(F32)
    return first, second, rest - second


def kernel(ls_ref, os_ref, w_hbm, z_hbm, x_hbm, v_hbm, o_ref,
           w_ref, zin, xs, vs, xaug, zall, ysend, yrecv, own,
           in_sem, zs_sem, zr_sem, ys_sem, yr_sem):
    me = lax.axis_index("sp")
    dp = lax.axis_index("dp")
    my_core, my_x, my_y = me % 2, (me // 2) % 2, me // 4

    def peer(k):
        c = (my_core + k % 2) % 2
        x = (my_x + (k // 2) % 2) % 2
        y = (my_y + k // 4) % 2
        return (y * 2 + x) * 2 + c

    zcopy = pltpu.make_async_copy(z_hbm, zin, in_sem.at[0])
    xcopy = pltpu.make_async_copy(x_hbm, xs, in_sem.at[1])
    vcopy = pltpu.make_async_copy(v_hbm, vs, in_sem.at[2])
    wcopy = pltpu.make_async_copy(w_hbm, w_ref, in_sem.at[3])
    zcopy.start()
    xcopy.start()
    vcopy.start()
    wcopy.start()
    barrier = pltpu.get_barrier_semaphore()
    for k in range(1, 8):
        pl.semaphore_signal(barrier, inc=1, device_id=(dp, peer(k)), device_id_type=pl.DeviceIdType.MESH)

    lv = jnp.full((8, 128), ls_ref[0], F32)
    l2 = lv * lv
    pv = jnp.where(l2 > 2.0**64, 2.0**-64, 1.0)
    l2p = l2 * pv
    cvec = LOG2E / l2p
    lns = l2p * jnp.log(jnp.full((8, 128), os_ref[0], F32))
    c = cvec[0, 0]
    s = os_ref[0].astype(BF16)
    sub = lax.broadcasted_iota(jnp.int32, (16, 128), 0)

    zcopy.wait()
    for q in range(4):
        zt = zin[pl.ds(128 * q, 128), :].astype(F32).T
        nz = jnp.sum(zt * zt, axis=0, keepdims=True)
        r = jnp.broadcast_to(nz, (16, 128)) * (-0.5 * pv[0:1, :]) + lns[0:1, :]
        a, b, d = limbs(r)
        aug = jnp.where(sub < 3, 1.0, jnp.where(sub == 3, a, jnp.where(sub == 4, b, jnp.where(sub == 5, d, 0.0))))
        zall[0, q, 0:128, :] = (zt * pv[0:1, :]).astype(BF16)
        zall[0, q, 128:144, :] = aug.astype(BF16)

    def zsend(k):
        return pltpu.make_async_remote_copy(
            src_ref=zall.at[0], dst_ref=zall.at[k], send_sem=zs_sem.at[k - 1], recv_sem=zr_sem.at[k - 1],
            device_id=(dp, peer(k)), device_id_type=pl.DeviceIdType.MESH)

    def ycopy(k):
        return pltpu.make_async_remote_copy(
            src_ref=ysend.at[k - 1], dst_ref=yrecv.at[k - 1], send_sem=ys_sem.at[k - 1], recv_sem=yr_sem.at[k - 1],
            device_id=(dp, peer(k)), device_id_type=pl.DeviceIdType.MESH)

    n_src = xs.shape[0]
    lane = lax.broadcasted_iota(jnp.int32, (TILE, 128), 1)

    def prep(i, carry):
        r0 = pl.multiple_of(i * TILE, TILE)
        xf = xs[pl.ds(r0, TILE), :].astype(F32)
        nx = jnp.sum(xf * xf, axis=1, keepdims=True)
        r = jnp.broadcast_to(nx, (TILE, 128)) * (-0.5 * pv[0:1, :])
        a, b, d = limbs(r)
        aug = jnp.where(lane == 0, a, jnp.where(lane == 1, b, jnp.where(lane == 2, d, jnp.where(lane < 6, 1.0, 0.0))))
        xaug[pl.ds(r0, TILE), :] = aug.astype(BF16)
        return carry

    def segment(slot, r0, r1):
        rhs = jnp.concatenate([zall[slot, q] for q in range(4)], axis=1)
        acc = jnp.zeros((16, 512), F32)
        for at in range(r0, r1, CHUNK):
            lhs = jnp.concatenate([xs[at:at + CHUNK, :], xaug[at:at + CHUNK, :]], axis=1)[:, :ZROWS]
            t = jnp.dot(lhs, rhs, preferred_element_type=F32)
            kern = jnp.minimum(jnp.exp2(t * c).astype(BF16), s)
            acc = acc + jnp.dot(vs[:, at:at + CHUNK], kern, preferred_element_type=F32)
        return acc

    half = n_src // 2
    xcopy.wait()
    lax.fori_loop(0, half // TILE, prep, 0)
    pl.semaphore_wait(barrier, 7)
    for k in ORDER:
        zsend(k).start()
    lax.fori_loop(half // TILE, n_src // TILE, prep, 0)
    vcopy.wait()
    own[...] = segment(0, 0, half)

    def one(i, table):
        k = table % 8
        zsend(k).wait_recv()
        ysend[k - 1] = segment(k, 0, n_src)
        ycopy(k).start()
        return table // 8

    lax.fori_loop(0, 7, one, sum(k * 8**i for i, k in enumerate(ORDER)))
    own[...] += segment(0, half, n_src)
    wcopy.wait()
    total = own[...] * w_ref[0, me].astype(F32)
    for k in ORDER:
        ycopy(k).wait_recv()
        total = total + yrecv[k - 1] * w_ref[0, peer(k)].astype(F32)
    o_ref[...] = total
    for k in ORDER:
        zsend(k).wait_send()
        ycopy(k).wait_send()


def solution(mesh):
    row_spec = P(("dp", "sp"), None)

    def local_fn(z_rows, x_rows, v_rows, mask_row, length_scale, out_scale):
        n_src, r_cols = v_rows.shape
        n_tgt, depth = z_rows.shape
        smem = pl.BlockSpec(memory_space=pltpu.SMEM)
        anywhere = pl.BlockSpec(memory_space=pltpu.HBM)
        y_t = pl.pallas_call(
            kernel,
            out_shape=jax.ShapeDtypeStruct((r_cols, n_tgt), F32),
            in_specs=[smem, smem, anywhere, anywhere, anywhere, anywhere],
            out_specs=pl.BlockSpec(memory_space=pltpu.VMEM),
            scratch_shapes=[
                pltpu.SMEM(mask_row.shape, jnp.int32),
                pltpu.VMEM((n_tgt, depth), BF16),
                pltpu.VMEM((n_src, depth), BF16),
                pltpu.VMEM((r_cols, n_src), BF16),
                pltpu.VMEM((n_src, 128), BF16),
                pltpu.VMEM((8, 4, ZROWS, 128), BF16),
                pltpu.VMEM((7, r_cols, n_tgt), F32),
                pltpu.VMEM((7, r_cols, n_tgt), F32),
                pltpu.VMEM((r_cols, n_tgt), F32),
                pltpu.SemaphoreType.DMA((4,)),
                pltpu.SemaphoreType.DMA((7,)),
                pltpu.SemaphoreType.DMA((7,)),
                pltpu.SemaphoreType.DMA((7,)),
                pltpu.SemaphoreType.DMA((7,)),
            ],
            compiler_params=pltpu.CompilerParams(
                collective_id=0, has_side_effects=True, vmem_limit_bytes=60 * 2**20),
        )(length_scale, out_scale, mask_row, z_rows, x_rows, v_rows.T)
        return y_t.T

    return jax.shard_map(local_fn, mesh=mesh, in_specs=(row_spec, row_spec, row_spec, row_spec, P(None), P(None)),
                         out_specs=row_spec, check_vma=False)
```

```python
import jax
import jax.numpy as jnp
from jax import lax
from jax.experimental import pallas as pl
from jax.experimental.pallas import tpu as pltpu
from jax.sharding import PartitionSpec as P

F32 = jnp.float32
BF16 = jnp.bfloat16
LOG2E = 1.4426950408889634
PREP = 2048
CHUNK = 4096
TILE = 256
ZROWS = 144
MESH = pl.DeviceIdType.MESH


def limbs(r):
    first = r.astype(BF16).astype(F32)
    rest = jnp.where(jnp.abs(first) < jnp.inf, r - first, 0.0)
    second = rest.astype(BF16).astype(F32)
    return first, second, rest - second


def scalars(ls_ref, os_ref):
    lv = jnp.full((8, 128), ls_ref[0], F32)
    l2 = lv * lv
    pv = jnp.where(l2 > 2.0**64, 2.0**-64, 1.0)
    l2p = l2 * pv
    return pv, LOG2E / l2p, l2p * jnp.log(jnp.full((8, 128), os_ref[0], F32))


def peer(me, k):
    c = (me % 2 + k % 2) % 2
    x = ((me // 2) % 2 + (k // 2) % 2) % 2
    y = (me // 4 + k // 4) % 2
    return (y * 2 + x) * 2 + c


def gather_kernel(ls_ref, os_ref, w_hbm, z_hbm, x_hbm, v_hbm, xs, xaug, vs, zall, own,
                  w_ref, zin, in_sem, zs_sem, zr_sem, xs_sem, xr_sem):
    me = lax.axis_index("sp")
    dp = lax.axis_index("dp")
    zcopy = pltpu.make_async_copy(z_hbm, zin, in_sem.at[0])
    xcopy = pltpu.make_async_copy(x_hbm, xs.at[0], in_sem.at[1])
    vcopy = pltpu.make_async_copy(v_hbm, vs.at[0], in_sem.at[2])
    wcopy = pltpu.make_async_copy(w_hbm, w_ref, in_sem.at[3])
    zcopy.start()
    wcopy.start()
    xcopy.start()
    vcopy.start()
    barrier = pltpu.get_barrier_semaphore()
    for k in (1, 2, 4, 6):
        pl.semaphore_signal(barrier, inc=1, device_id=(dp, peer(me, k)), device_id_type=MESH)

    pv, cvec, lns = scalars(ls_ref, os_ref)
    c = cvec[0, 0]
    s = os_ref[0].astype(BF16)
    sub = lax.broadcasted_iota(jnp.int32, (16, 128), 0)
    lane = lax.broadcasted_iota(jnp.int32, (16, 128), 1)
    wcopy.wait()
    bits = jnp.zeros((16, 128), F32)
    for j in range(8):
        bits = jnp.where(lane == j, w_ref[0, j].astype(F32), bits)
    zcopy.wait()
    for q in range(4):
        zt = zin[pl.ds(128 * q, 128), :].astype(F32).T
        nz = jnp.sum(zt * zt, axis=0, keepdims=True)
        a, b, d = limbs(jnp.broadcast_to(nz, (16, 128)) * (-0.5 * pv[0:1, :]) + lns[0:1, :])
        aug = jnp.where(sub < 3, 1.0, jnp.where(sub == 3, a, jnp.where(sub == 4, b, jnp.where(
            sub == 5, d, jnp.where(sub == 6, bits, 0.0)))))
        zall[0, q, 0:128, :] = (zt * pv[0:1, :]).astype(BF16)
        zall[0, q, 128:144, :] = aug.astype(BF16)

    def zcopy_to(n, src, dst, h, k):
        return pltpu.make_async_remote_copy(
            src_ref=zall.at[src, pl.ds(2 * h, 2)], dst_ref=zall.at[dst, pl.ds(2 * h, 2)],
            send_sem=zs_sem.at[n], recv_sem=zr_sem.at[n], device_id=(dp, peer(me, k)), device_id_type=MESH)

    copies = {name: zcopy_to(n, *name) for n, name in enumerate((
        (0, 1, 0, 2), (0, 2, 1, 4), (0, 1, 1, 2), (0, 2, 0, 4), (1, 3, 0, 4), (2, 3, 1, 2)))}
    xsend = pltpu.make_async_remote_copy(
        src_ref=x_hbm, dst_ref=xs.at[1], send_sem=xs_sem.at[0], recv_sem=xr_sem.at[0],
        device_id=(dp, peer(me, 1)), device_id_type=MESH)
    vsend = pltpu.make_async_remote_copy(
        src_ref=v_hbm, dst_ref=vs.at[1], send_sem=xs_sem.at[1], recv_sem=xr_sem.at[1],
        device_id=(dp, peer(me, 1)), device_id_type=MESH)

    n_src = xs.shape[1]
    ones = jnp.ones((16, 256), BF16)

    def prep(which):
        def body(i, carry):
            r0 = pl.multiple_of(i * PREP, PREP)
            xf = xs[which, pl.ds(r0, PREP), :].astype(F32)
            sq = xf * xf
            hi = sq.astype(BF16)
            lo = (sq - hi.astype(F32)).astype(BF16)
            nx = lax.dot_general(ones, jnp.concatenate([hi, lo], axis=1), (((1,), (1,)), ((), ())),
                                 preferred_element_type=F32)
            for h in range(PREP // 128):
                a, b, d = limbs(nx[:, 128 * h:128 * h + 128] * (-0.5 * pv[0:1, :]))
                aug = jnp.where(sub == 0, a, jnp.where(sub == 1, b, jnp.where(sub == 2, d, jnp.where(
                    sub < 6, 1.0, 0.0))))
                full = jnp.concatenate([aug.astype(BF16), jnp.zeros((112, 128), BF16)], axis=0)
                xaug[which, pl.ds(r0 + 128 * h, 128), :] = full.T
            return carry
        lax.fori_loop(0, n_src // PREP, body, 0)

    def piece(at):
        rhs = jnp.concatenate([zall[0, q] for q in range(4)], axis=1)
        lhs = jnp.concatenate([xs[0, at:at + CHUNK, :], xaug[0, at:at + CHUNK, :]], axis=1)[:, :ZROWS]
        t = jnp.dot(lhs, rhs, preferred_element_type=F32)
        kern = jnp.minimum(jnp.exp2(t * c).astype(BF16), s)
        return jnp.dot(vs[0, :, at:at + CHUNK], kern, preferred_element_type=F32)

    def pass_on(got, onward):
        copies[got].wait_recv()
        copies[onward].start()

    pl.semaphore_wait(barrier, 4)
    for name in copies:
        if name[0] == 0:
            copies[name].start()
    xsend.start()
    vsend.start()
    xcopy.wait()
    prep(0)
    vcopy.wait()
    own[...] = piece(0)
    pass_on((0, 1, 0, 2), (1, 3, 0, 4))
    pass_on((0, 2, 1, 4), (2, 3, 1, 2))
    for at in range(CHUNK, n_src, CHUNK):
        own[...] += piece(at)
    xsend.wait_recv()
    prep(1)
    vsend.wait_recv()
    for name in ((0, 1, 1, 2), (0, 2, 0, 4), (1, 3, 0, 4), (2, 3, 1, 2)):
        copies[name].wait_recv()
    for copy in (*copies.values(), xsend, vsend):
        copy.wait_send()


def block_kernel(ls_ref, os_ref, xs, xaug, vs, zall, own, y_ref, flags):
    me = lax.axis_index("sp")
    _, cvec, _ = scalars(ls_ref, os_ref)
    c = cvec[0, 0]
    s = os_ref[0].astype(BF16)
    n_tiles = xs.shape[1] // TILE
    sub = lax.broadcasted_iota(jnp.int32, (16, 128), 0)
    lane = lax.broadcasted_iota(jnp.int32, (16, 128), 1)
    for slot in range(4):
        bits = zall[slot, 0, 128:144, :].astype(F32)
        for src in range(2):
            hit = (sub == 6) & (lane == (me + src * (1 - 2 * (me % 2))))
            flags[2 * slot + src] = jnp.sum(jnp.where(hit, bits, 0.0)).astype(jnp.int32)
    y_ref[0] = own[...]
    for slot in range(1, 4):
        y_ref[slot] = jnp.zeros_like(own)

    def main(*accs):
        g_acc = (accs[0:3], accs[3:6])
        y_acc = accs[6:8]
        zero_rows = jnp.zeros((256 - ZROWS, 256), BF16)

        def block(slot, src):
            def first(j):
                for m in range(2):
                    rows = jnp.concatenate([zall[slot, 2 * m], zall[slot, 2 * m + 1]], axis=1)
                    pltpu.matmul_push_rhs(jnp.concatenate([rows, zero_rows], axis=0), staging_register=0, mxu_index=m)
                at = pl.ds(j * TILE, TILE)
                lhs = jnp.concatenate([xs[src, at, :], xaug[src, at, :]], axis=1)
                for m in range(2):
                    pltpu.matmul_acc_lhs(g_acc[m][j % 3], lhs, load_staged_rhs=0)

            def second(j):
                for m in range(2):
                    t = pltpu.matmul_pop(g_acc[m][j % 3])
                    kern = jnp.minimum(jnp.exp2(t * c).astype(BF16), s)
                    pltpu.matmul_push_rhs(kern, staging_register=1, mxu_index=m)
                for m in range(2):
                    pltpu.matmul_acc_lhs(y_acc[m], vs[src, :, pl.ds(j * TILE, TILE)], load_staged_rhs=1)

            for j in range(n_tiles):
                first(j)
                if j >= 2:
                    second(j - 2)
            second(n_tiles - 2)
            second(n_tiles - 1)
            for m in range(2):
                y_ref[slot, :, 256 * m:256 * m + 256] += pltpu.matmul_pop(y_acc[m])

        def one(e, carry):
            @pl.when(flags[e] != 0)
            def _():
                block(e // 2, e % 2)
            return carry

        lax.fori_loop(1, 8, one, 0)

    big = [pltpu.ACC(m)((TILE, 256), F32) for m in (0, 0, 0, 1, 1, 1)]
    small = [pltpu.ACC(m)((16, 256), F32) for m in (0, 1)]
    pl.run_scoped(main, *big, *small)


def sum_kernel(y_ref, o_ref, yrecv, s_sem, r_sem):
    me = lax.axis_index("sp")
    dp = lax.axis_index("dp")
    barrier = pltpu.get_barrier_semaphore()
    for k in (2, 4, 6):
        pl.semaphore_signal(barrier, inc=1, device_id=(dp, peer(me, k)), device_id_type=MESH)
    pl.semaphore_wait(barrier, 3)
    copies = [pltpu.make_async_remote_copy(
        src_ref=y_ref.at[n + 1], dst_ref=yrecv.at[n], send_sem=s_sem.at[n], recv_sem=r_sem.at[n],
        device_id=(dp, peer(me, 2 * n + 2)), device_id_type=MESH) for n in (2, 0, 1)]
    for copy in copies:
        copy.start()
    for copy in copies:
        copy.wait_recv()
    o_ref[...] = (y_ref[0] + yrecv[0]) + (yrecv[1] + yrecv[2])
    for copy in copies:
        copy.wait_send()


def solution(mesh):
    row_spec = P(("dp", "sp"), None)
    smem = pl.BlockSpec(memory_space=pltpu.SMEM)
    hbm = pl.BlockSpec(memory_space=pltpu.HBM)
    vmem = pl.BlockSpec(memory_space=pltpu.VMEM)
    dma = pltpu.SemaphoreType.DMA

    def local_fn(z_rows, x_rows, v_rows, mask_row, length_scale, out_scale):
        n_src, r_cols = v_rows.shape
        n_tgt, depth = z_rows.shape
        gathered = pl.pallas_call(
            gather_kernel,
            out_shape=[
                jax.ShapeDtypeStruct((2, n_src, depth), BF16),
                jax.ShapeDtypeStruct((2, n_src, 128), BF16),
                jax.ShapeDtypeStruct((2, r_cols, n_src), BF16),
                jax.ShapeDtypeStruct((4, 4, ZROWS, 128), BF16),
                jax.ShapeDtypeStruct((r_cols, n_tgt), F32),
            ],
            in_specs=[smem, smem, hbm, hbm, hbm, hbm],
            out_specs=[vmem] * 5,
            scratch_shapes=[
                pltpu.SMEM(mask_row.shape, jnp.int32),
                pltpu.VMEM((n_tgt, depth), BF16),
                dma((4,)), dma((6,)), dma((6,)), dma((2,)), dma((2,)),
            ],
            compiler_params=pltpu.CompilerParams(
                collective_id=0, has_side_effects=True, vmem_limit_bytes=int(54.5 * 2**20)),
        )(length_scale, out_scale, mask_row, z_rows, x_rows, v_rows.T)
        partial = pl.pallas_call(
            block_kernel,
            out_shape=jax.ShapeDtypeStruct((4, r_cols, n_tgt), F32),
            in_specs=[smem, smem] + [vmem] * 5,
            out_specs=vmem,
            scratch_shapes=[pltpu.SMEM((8,), jnp.int32)],
            compiler_params=pltpu.CompilerParams(vmem_limit_bytes=20 * 2**20),
        )(length_scale, out_scale, *gathered)
        y_t = pl.pallas_call(
            sum_kernel,
            out_shape=jax.ShapeDtypeStruct((r_cols, n_tgt), F32),
            in_specs=[vmem],
            out_specs=vmem,
            scratch_shapes=[pltpu.VMEM((3, r_cols, n_tgt), F32), dma((3,)), dma((3,))],
            compiler_params=pltpu.CompilerParams(
                collective_id=1, has_side_effects=True, vmem_limit_bytes=20 * 2**20),
        )(partial)
        return y_t.T

    return jax.shard_map(local_fn, mesh=mesh, in_specs=(row_spec, row_spec, row_spec, row_spec, P(None), P(None)),
                         out_specs=row_spec, check_vma=False)
```

```python
import jax
import jax.numpy as jnp
from jax import lax
from jax.experimental import pallas as pl
from jax.experimental.pallas import tpu as pltpu
from jax.sharding import PartitionSpec as P

F32 = jnp.float32
BF16 = jnp.bfloat16
LOG2E = 1.4426950408889634
PREP = 2048
CHUNK = 4096
TILE = 256
ZROWS = 144
MESH = pl.DeviceIdType.MESH


def limbs(r):
    first = r.astype(BF16).astype(F32)
    rest = jnp.where(jnp.abs(first) < jnp.inf, r - first, 0.0)
    second = rest.astype(BF16).astype(F32)
    return first, second, rest - second


def scalars(ls_ref, os_ref):
    lv = jnp.full((8, 128), ls_ref[0], F32)
    l2 = lv * lv
    pv = jnp.where(l2 > 2.0**64, 2.0**-64, 1.0)
    l2p = l2 * pv
    return pv, LOG2E / l2p, l2p * jnp.log(jnp.full((8, 128), os_ref[0], F32))


def peer(me, k):
    c = (me % 2 + k % 2) % 2
    x = ((me // 2) % 2 + (k // 2) % 2) % 2
    y = (me // 4 + k // 4) % 2
    return (y * 2 + x) * 2 + c


def gather_kernel(ls_ref, os_ref, w_hbm, z_hbm, x_hbm, v_hbm, xs, xaug, vs, zall, own,
                  w_ref, zin, in_sem, zs_sem, zr_sem, xs_sem, xr_sem):
    me = lax.axis_index("sp")
    dp = lax.axis_index("dp")
    zcopy = pltpu.make_async_copy(z_hbm, zin, in_sem.at[0])
    xcopy = pltpu.make_async_copy(x_hbm, xs.at[0], in_sem.at[1])
    vcopy = pltpu.make_async_copy(v_hbm, vs.at[0], in_sem.at[2])
    wcopy = pltpu.make_async_copy(w_hbm, w_ref, in_sem.at[3])
    zcopy.start()
    wcopy.start()
    xcopy.start()
    vcopy.start()
    barrier = pltpu.get_barrier_semaphore()
    for k in (1, 2, 4, 6):
        pl.semaphore_signal(barrier, inc=1, device_id=(dp, peer(me, k)), device_id_type=MESH)

    pv, cvec, lns = scalars(ls_ref, os_ref)
    c = cvec[0, 0]
    s = os_ref[0].astype(BF16)
    sub = lax.broadcasted_iota(jnp.int32, (16, 128), 0)
    lane = lax.broadcasted_iota(jnp.int32, (16, 128), 1)
    wcopy.wait()
    bits = jnp.zeros((16, 128), F32)
    for j in range(8):
        bits = jnp.where(lane == j, w_ref[0, j].astype(F32), bits)
    zcopy.wait()
    for q in range(4):
        zt = zin[pl.ds(128 * q, 128), :].astype(F32).T
        nz = jnp.sum(zt * zt, axis=0, keepdims=True)
        a, b, d = limbs(jnp.broadcast_to(nz, (16, 128)) * (-0.5 * pv[0:1, :]) + lns[0:1, :])
        aug = jnp.where(sub < 3, 1.0, jnp.where(sub == 3, a, jnp.where(sub == 4, b, jnp.where(
            sub == 5, d, jnp.where(sub == 6, bits, 0.0)))))
        zall[0, q, 0:128, :] = (zt * pv[0:1, :]).astype(BF16)
        zall[0, q, 128:144, :] = aug.astype(BF16)

    def zcopy_to(n, src, dst, h, k):
        return pltpu.make_async_remote_copy(
            src_ref=zall.at[src, pl.ds(2 * h, 2)], dst_ref=zall.at[dst, pl.ds(2 * h, 2)],
            send_sem=zs_sem.at[n], recv_sem=zr_sem.at[n], device_id=(dp, peer(me, k)), device_id_type=MESH)

    copies = {name: zcopy_to(n, *name) for n, name in enumerate((
        (0, 1, 0, 2), (0, 2, 1, 4), (0, 1, 1, 2), (0, 2, 0, 4), (1, 3, 0, 4), (2, 3, 1, 2)))}
    xsend = pltpu.make_async_remote_copy(
        src_ref=x_hbm, dst_ref=xs.at[1], send_sem=xs_sem.at[0], recv_sem=xr_sem.at[0],
        device_id=(dp, peer(me, 1)), device_id_type=MESH)
    vsend = pltpu.make_async_remote_copy(
        src_ref=v_hbm, dst_ref=vs.at[1], send_sem=xs_sem.at[1], recv_sem=xr_sem.at[1],
        device_id=(dp, peer(me, 1)), device_id_type=MESH)

    n_src = xs.shape[1]
    ones = jnp.ones((16, 256), BF16)

    def prep(which):
        def body(i, carry):
            r0 = pl.multiple_of(i * PREP, PREP)
            xf = xs[which, pl.ds(r0, PREP), :].astype(F32)
            sq = xf * xf
            hi = sq.astype(BF16)
            lo = (sq - hi.astype(F32)).astype(BF16)
            nx = lax.dot_general(ones, jnp.concatenate([hi, lo], axis=1), (((1,), (1,)), ((), ())),
                                 preferred_element_type=F32)
            for h in range(PREP // 128):
                a, b, d = limbs(nx[:, 128 * h:128 * h + 128] * (-0.5 * pv[0:1, :]))
                aug = jnp.where(sub == 0, a, jnp.where(sub == 1, b, jnp.where(sub == 2, d, jnp.where(
                    sub < 6, 1.0, 0.0))))
                full = jnp.concatenate([aug.astype(BF16), jnp.zeros((112, 128), BF16)], axis=0)
                xaug[which, pl.ds(r0 + 128 * h, 128), :] = full.T
            return carry
        lax.fori_loop(0, n_src // PREP, body, 0)

    def piece(at):
        rhs = jnp.concatenate([zall[0, q] for q in range(4)], axis=1)
        lhs = jnp.concatenate([xs[0, at:at + CHUNK, :], xaug[0, at:at + CHUNK, :]], axis=1)[:, :ZROWS]
        t = jnp.dot(lhs, rhs, preferred_element_type=F32)
        kern = jnp.minimum(jnp.exp2(t * c).astype(BF16), s)
        return jnp.dot(vs[0, :, at:at + CHUNK], kern, preferred_element_type=F32)

    def pass_on(got, onward):
        copies[got].wait_recv()
        copies[onward].start()

    pl.semaphore_wait(barrier, 4)
    for name in copies:
        if name[0] == 0:
            copies[name].start()
    xsend.start()
    vsend.start()
    xcopy.wait()
    prep(0)
    vcopy.wait()
    own[...] = piece(0)
    pass_on((0, 1, 0, 2), (1, 3, 0, 4))
    pass_on((0, 2, 1, 4), (2, 3, 1, 2))
    for at in range(CHUNK, n_src, CHUNK):
        own[...] += piece(at)
    xsend.wait_recv()
    prep(1)
    vsend.wait_recv()
    for name in ((0, 1, 1, 2), (0, 2, 0, 4), (1, 3, 0, 4), (2, 3, 1, 2)):
        copies[name].wait_recv()
    for copy in (*copies.values(), xsend, vsend):
        copy.wait_send()


def block_kernel(ls_ref, os_ref, xs, xaug, vs, zall, own, y_ref, flags):
    me = lax.axis_index("sp")
    _, cvec, _ = scalars(ls_ref, os_ref)
    c = cvec[0, 0]
    s = os_ref[0].astype(BF16)
    n_tiles = xs.shape[1] // TILE
    sub = lax.broadcasted_iota(jnp.int32, (16, 128), 0)
    lane = lax.broadcasted_iota(jnp.int32, (16, 128), 1)
    for slot in range(4):
        bits = zall[slot, 0, 128:144, :].astype(F32)
        for src in range(2):
            hit = (sub == 6) & (lane == (me + src * (1 - 2 * (me % 2))))
            flags[2 * slot + src] = jnp.sum(jnp.where(hit, bits, 0.0)).astype(jnp.int32)
    y_ref[0] = own[...]
    for slot in range(1, 4):
        y_ref[slot] = jnp.zeros_like(own)

    def main(*accs):
        g_acc = (accs[0:3], accs[3:6])
        y_acc = accs[6:8]
        zero_rows = jnp.zeros((256 - ZROWS, 256), BF16)

        def block(slot, src):
            def first(j):
                for m in range(2):
                    rows = jnp.concatenate([zall[slot, 2 * m], zall[slot, 2 * m + 1]], axis=1)
                    pltpu.matmul_push_rhs(jnp.concatenate([rows, zero_rows], axis=0), staging_register=0, mxu_index=m)
                at = pl.ds(j * TILE, TILE)
                lhs = jnp.concatenate([xs[src, at, :], xaug[src, at, :]], axis=1)
                for m in range(2):
                    pltpu.matmul_acc_lhs(g_acc[m][j % 3], lhs, load_staged_rhs=0)

            def second(j):
                for m in range(2):
                    t = pltpu.matmul_pop(g_acc[m][j % 3])
                    kern = jnp.minimum(jnp.exp2(t * c).astype(BF16), s)
                    pltpu.matmul_push_rhs(kern, staging_register=1, mxu_index=m)
                for m in range(2):
                    pltpu.matmul_acc_lhs(y_acc[m], vs[src, :, pl.ds(j * TILE, TILE)], load_staged_rhs=1)

            for j in range(n_tiles):
                first(j)
                if j >= 2:
                    second(j - 2)
            second(n_tiles - 2)
            second(n_tiles - 1)
            for m in range(2):
                y_ref[slot, :, 256 * m:256 * m + 256] += pltpu.matmul_pop(y_acc[m])

        def one(e, carry):
            @pl.when(flags[e] != 0)
            def _():
                block(e // 2, e % 2)
            return carry

        lax.fori_loop(1, 8, one, 0)

    big = [pltpu.ACC(m)((TILE, 256), F32) for m in (0, 0, 0, 1, 1, 1)]
    small = [pltpu.ACC(m)((16, 256), F32) for m in (0, 1)]
    pl.run_scoped(main, *big, *small)


def sum_kernel(y_ref, o_ref, yrecv, s_sem, r_sem):
    me = lax.axis_index("sp")
    dp = lax.axis_index("dp")
    barrier = pltpu.get_barrier_semaphore()
    for k in (2, 4, 6):
        pl.semaphore_signal(barrier, inc=1, device_id=(dp, peer(me, k)), device_id_type=MESH)
    pl.semaphore_wait(barrier, 3)
    copies = [pltpu.make_async_remote_copy(
        src_ref=y_ref.at[n + 1], dst_ref=yrecv.at[n], send_sem=s_sem.at[n], recv_sem=r_sem.at[n],
        device_id=(dp, peer(me, 2 * n + 2)), device_id_type=MESH) for n in (2, 0, 1)]
    for copy in copies:
        copy.start()
    for copy in copies:
        copy.wait_recv()
    o_ref[...] = (y_ref[0] + yrecv[0]) + (yrecv[1] + yrecv[2])
    for copy in copies:
        copy.wait_send()


def solution(mesh):
    row_spec = P(("dp", "sp"), None)
    smem = pl.BlockSpec(memory_space=pltpu.SMEM)
    hbm = pl.BlockSpec(memory_space=pltpu.HBM)
    vmem = pl.BlockSpec(memory_space=pltpu.VMEM)
    dma = pltpu.SemaphoreType.DMA

    def local_fn(z_rows, x_rows, v_rows, mask_row, length_scale, out_scale):
        n_src, r_cols = v_rows.shape
        n_tgt, depth = z_rows.shape
        gathered = pl.pallas_call(
            gather_kernel,
            out_shape=[
                jax.ShapeDtypeStruct((2, n_src, depth), BF16),
                jax.ShapeDtypeStruct((2, n_src, 128), BF16),
                jax.ShapeDtypeStruct((2, r_cols, n_src), BF16),
                jax.ShapeDtypeStruct((4, 4, ZROWS, 128), BF16),
                jax.ShapeDtypeStruct((r_cols, n_tgt), F32),
            ],
            in_specs=[smem, smem, hbm, hbm, hbm, hbm],
            out_specs=[vmem] * 5,
            scratch_shapes=[
                pltpu.SMEM(mask_row.shape, jnp.int32),
                pltpu.VMEM((n_tgt, depth), BF16),
                dma((4,)), dma((6,)), dma((6,)), dma((2,)), dma((2,)),
            ],
            compiler_params=pltpu.CompilerParams(
                collective_id=0, has_side_effects=True, vmem_limit_bytes=40 * 2**20),
        )(length_scale, out_scale, *[pltpu.with_memory_space_constraint(a, pltpu.HBM) for a in (mask_row, z_rows, x_rows, v_rows.T)])
        partial = pl.pallas_call(
            block_kernel,
            out_shape=jax.ShapeDtypeStruct((4, r_cols, n_tgt), F32),
            in_specs=[smem, smem] + [vmem] * 5,
            out_specs=vmem,
            scratch_shapes=[pltpu.SMEM((8,), jnp.int32)],
            compiler_params=pltpu.CompilerParams(vmem_limit_bytes=20 * 2**20),
        )(length_scale, out_scale, *gathered)
        y_t = pl.pallas_call(
            sum_kernel,
            out_shape=jax.ShapeDtypeStruct((r_cols, n_tgt), F32),
            in_specs=[vmem],
            out_specs=vmem,
            scratch_shapes=[pltpu.VMEM((3, r_cols, n_tgt), F32), dma((3,)), dma((3,))],
            compiler_params=pltpu.CompilerParams(
                collective_id=1, has_side_effects=True, vmem_limit_bytes=20 * 2**20),
        )(partial)
        return y_t.T

    return jax.shard_map(local_fn, mesh=mesh, in_specs=(row_spec, row_spec, row_spec, row_spec, P(None), P(None)),
                         out_specs=row_spec, check_vma=False)
```

```python
import jax
import jax.numpy as jnp
from jax import lax
from jax.experimental import pallas as pl
from jax.experimental.pallas import tpu as pltpu
from jax.sharding import PartitionSpec as P

F32 = jnp.float32
BF16 = jnp.bfloat16
LOG2E = 1.4426950408889634
PREP = 8192
EARLY = 4096
LATE = 0
TILE = 256
ZROWS = 144
MESH = pl.DeviceIdType.MESH


def limbs(r):
    first = r.astype(BF16).astype(F32)
    rest = jnp.where(jnp.abs(first) < jnp.inf, r - first, 0.0)
    second = rest.astype(BF16).astype(F32)
    return first, second, rest - second


def scalars(ls_ref, os_ref):
    lv = jnp.full((8, 128), ls_ref[0], F32)
    l2 = lv * lv
    pv = jnp.where(l2 > 2.0**64, 2.0**-64, 1.0)
    l2p = l2 * pv
    return pv, LOG2E / l2p, l2p * jnp.log(jnp.full((8, 128), os_ref[0], F32))


def peer(me, k):
    c = (me % 2 + k % 2) % 2
    x = ((me // 2) % 2 + (k // 2) % 2) % 2
    y = (me // 4 + k // 4) % 2
    return (y * 2 + x) * 2 + c


def piece(z_slot, src, at, rows, c, s, xs, xaug, vs, zall):
    rhs = jnp.concatenate([zall[z_slot, q] for q in range(4)], axis=1)
    lhs = jnp.concatenate([xs[src, at:at + rows, :], xaug[src, at:at + rows, :]], axis=1)[:, :ZROWS]
    t = jnp.dot(lhs, rhs, preferred_element_type=F32)
    kern = jnp.minimum(jnp.exp2(t * c).astype(BF16), s)
    return jnp.dot(vs[src, :, at:at + rows], kern, preferred_element_type=F32)


def mask_bit(zall, slot, dev):
    sub = lax.broadcasted_iota(jnp.int32, (16, 128), 0)
    lane = lax.broadcasted_iota(jnp.int32, (16, 128), 1)
    bits = jnp.where((sub == 6) & (lane == dev), zall[slot, 0, 128:144, :].astype(F32), 0.0)
    return jnp.sum(jnp.sum(bits, axis=0, keepdims=True), axis=1, keepdims=True)


def gather_kernel(ls_ref, os_ref, w_hbm, z_hbm, x_hbm, v_hbm, xs, xaug, vs, zall, own,
                  w_ref, zin, in_sem, zs_sem, zr_sem, xs_sem, xr_sem):
    me = lax.axis_index("sp")
    dp = lax.axis_index("dp")
    zcopy = pltpu.make_async_copy(z_hbm, zin, in_sem.at[0])
    xcopy = pltpu.make_async_copy(x_hbm, xs.at[0], in_sem.at[1])
    vcopy = pltpu.make_async_copy(v_hbm, vs.at[0], in_sem.at[2])
    wcopy = pltpu.make_async_copy(w_hbm, w_ref, in_sem.at[3])
    zcopy.start()
    wcopy.start()
    xcopy.start()
    vcopy.start()
    barrier = pltpu.get_barrier_semaphore()
    for k in (1, 2, 4):
        pl.semaphore_signal(barrier, inc=1, device_id=(dp, peer(me, k)), device_id_type=MESH)

    pv, cvec, lns = scalars(ls_ref, os_ref)
    c = cvec[0, 0]
    s = os_ref[0].astype(BF16)
    sub = lax.broadcasted_iota(jnp.int32, (16, 128), 0)
    lane = lax.broadcasted_iota(jnp.int32, (16, 128), 1)
    wcopy.wait()
    bits = jnp.zeros((16, 128), F32)
    for j in range(8):
        bits = jnp.where(lane == j, w_ref[0, j].astype(F32), bits)
    zcopy.wait()
    for q in range(4):
        zt = zin[pl.ds(128 * q, 128), :].astype(F32).T
        nz = jnp.sum(zt * zt, axis=0, keepdims=True)
        a, b, d = limbs(jnp.broadcast_to(nz, (16, 128)) * (-0.5 * pv[0:1, :]) + lns[0:1, :])
        aug = jnp.where(sub < 3, 1.0, jnp.where(sub == 3, a, jnp.where(sub == 4, b, jnp.where(
            sub == 5, d, jnp.where(sub == 6, bits, 0.0)))))
        zall[0, q, 0:128, :] = (zt * pv[0:1, :]).astype(BF16)
        zall[0, q, 128:144, :] = aug.astype(BF16)

    def zcopy_to(n, src, dst, q, k):
        return pltpu.make_async_remote_copy(
            src_ref=zall.at[src, q], dst_ref=zall.at[dst, q],
            send_sem=zs_sem.at[n], recv_sem=zr_sem.at[n], device_id=(dp, peer(me, k)), device_id_type=MESH)

    order = tuple(zip((0, 1, 2, 3), (2, 3, 0, 1)))
    copies = {name: zcopy_to(n, *name) for n, name in enumerate(
        [one for q, r in order for one in ((0, 1, q, 2), (0, 2, r, 4))]
        + [(1, 3, 0, 4), (2, 3, 2, 2), (1, 3, 1, 4), (2, 3, 3, 2)])}
    xsend = pltpu.make_async_remote_copy(
        src_ref=x_hbm, dst_ref=xs.at[1], send_sem=xs_sem.at[0], recv_sem=xr_sem.at[0],
        device_id=(dp, peer(me, 1)), device_id_type=MESH)
    vsend = pltpu.make_async_remote_copy(
        src_ref=v_hbm, dst_ref=vs.at[1], send_sem=xs_sem.at[1], recv_sem=xr_sem.at[1],
        device_id=(dp, peer(me, 1)), device_id_type=MESH)

    n_src = xs.shape[1]
    ones = jnp.ones((16, 256), BF16)

    def prep(which):
        def body(i, carry):
            r0 = 0
            xf = xs[which, pl.ds(r0, PREP), :].astype(F32)
            sq = xf * xf
            hi = sq.astype(BF16)
            lo = (sq - hi.astype(F32)).astype(BF16)
            nx = lax.dot_general(ones, jnp.concatenate([hi, lo], axis=1), (((1,), (1,)), ((), ())),
                                 preferred_element_type=F32)
            for h in range(PREP // 128):
                a, b, d = limbs(nx[:, 128 * h:128 * h + 128] * (-0.5 * pv[0:1, :]))
                aug = jnp.where(sub == 0, a, jnp.where(sub == 1, b, jnp.where(sub == 2, d, jnp.where(
                    sub < 6, 1.0, 0.0))))
                full = jnp.concatenate([aug.astype(BF16), jnp.zeros((112, 128), BF16)], axis=0)
                xaug[which, pl.ds(r0 + 128 * h, 128), :] = full.T
            return carry
        body(0, 0)

    def pass_on(got, onward):
        copies[got].wait_recv()
        copies[onward].start()

    pl.semaphore_wait(barrier, 3)
    for name in copies:
        if name[0] == 0:
            copies[name].start()
    xsend.start()
    vsend.start()
    xcopy.wait()
    prep(0)
    vcopy.wait()
    first = piece(0, 0, 0, EARLY, c, s, xs, xaug, vs, zall)
    for q in (0, 1):
        pass_on((0, 1, q, 2), (1, 3, q, 4))
        pass_on((0, 2, q + 2, 4), (2, 3, q + 2, 2))
    xsend.wait_recv()
    prep(1)
    own[...] = first + piece(0, 0, EARLY, n_src - EARLY, c, s, xs, xaug, vs, zall)
    vsend.wait_recv()
    if LATE:
        extra = piece(0, 1, 0, LATE, c, s, xs, xaug, vs, zall)
        own[...] += extra * mask_bit(zall, 0, peer(me, 1))
    for q, r in order[2:]:
        copies[(0, 1, q, 2)].wait_recv()
        copies[(0, 2, r, 4)].wait_recv()
    for name in ((1, 3, 0, 4), (2, 3, 2, 2), (1, 3, 1, 4), (2, 3, 3, 2)):
        copies[name].wait_recv()
    for copy in (*copies.values(), xsend, vsend):
        copy.wait_send()


def block_kernel(ls_ref, os_ref, xs, xaug, vs, zall, own, y_ref, flags):
    me = lax.axis_index("sp")
    _, cvec, _ = scalars(ls_ref, os_ref)
    c = cvec[0, 0]
    s = os_ref[0].astype(BF16)
    n_tiles = xs.shape[1] // TILE
    for slot in range(1, 4):
        for src in range(2):
            flags[2 * slot + src] = mask_bit(zall, slot, peer(me, src))[0, 0].astype(jnp.int32)
    y_ref[0] = own[...]
    for slot in range(1, 4):
        y_ref[slot] = jnp.zeros_like(own)

    def main(*accs):
        g_acc = (accs[0:3], accs[3:6])
        y_acc = accs[6:8]
        zero_rows = jnp.zeros((256 - ZROWS, 256), BF16)

        def block(slot, src):
            def first(j):
                for m in range(2):
                    rows = jnp.concatenate([zall[slot, 2 * m], zall[slot, 2 * m + 1]], axis=1)
                    pltpu.matmul_push_rhs(jnp.concatenate([rows, zero_rows], axis=0), staging_register=0, mxu_index=m)
                at = pl.ds(j * TILE, TILE)
                lhs = jnp.concatenate([xs[src, at, :], xaug[src, at, :]], axis=1)
                for m in range(2):
                    pltpu.matmul_acc_lhs(g_acc[m][j % 3], lhs, load_staged_rhs=0)

            def second(j):
                for m in range(2):
                    t = pltpu.matmul_pop(g_acc[m][j % 3])
                    kern = jnp.minimum(jnp.exp2(t * c).astype(BF16), s)
                    pltpu.matmul_push_rhs(kern, staging_register=1, mxu_index=m)
                for m in range(2):
                    pltpu.matmul_acc_lhs(y_acc[m], vs[src, :, pl.ds(j * TILE, TILE)], load_staged_rhs=1)

            for j in range(n_tiles):
                first(j)
                if j >= 2:
                    second(j - 2)
            second(n_tiles - 2)
            second(n_tiles - 1)
            for m in range(2):
                y_ref[slot, :, 256 * m:256 * m + 256] += pltpu.matmul_pop(y_acc[m])

        def one(e, carry):
            @pl.when(flags[e] != 0)
            def _():
                block(e // 2, e % 2)
            return carry

        lax.fori_loop(2, 8, one, 0)

    big = [pltpu.ACC(m)((TILE, 256), F32) for m in (0, 0, 0, 1, 1, 1)]
    small = [pltpu.ACC(m)((16, 256), F32) for m in (0, 1)]
    pl.run_scoped(main, *big, *small)


def sum_kernel(ls_ref, os_ref, xs, xaug, vs, zall, y_ref, o_ref, yrecv, s_sem, r_sem):
    me = lax.axis_index("sp")
    dp = lax.axis_index("dp")
    barrier = pltpu.get_barrier_semaphore()
    for k in (2, 4, 6):
        pl.semaphore_signal(barrier, inc=1, device_id=(dp, peer(me, k)), device_id_type=MESH)
    pl.semaphore_wait(barrier, 3)
    copies = [pltpu.make_async_remote_copy(
        src_ref=y_ref.at[n + 1], dst_ref=yrecv.at[n], send_sem=s_sem.at[n], recv_sem=r_sem.at[n],
        device_id=(dp, peer(me, 2 * n + 2)), device_id_type=MESH) for n in (2, 0, 1)]
    for copy in copies:
        copy.start()
    _, cvec, _ = scalars(ls_ref, os_ref)
    rest = piece(0, 1, LATE, xs.shape[1] - LATE, cvec[0, 0], os_ref[0].astype(BF16), xs, xaug, vs, zall)
    own = y_ref[0] + rest * mask_bit(zall, 0, peer(me, 1))
    for copy in copies:
        copy.wait_recv()
    o_ref[...] = (own + yrecv[0]) + (yrecv[1] + yrecv[2])
    for copy in copies:
        copy.wait_send()


def solution(mesh):
    row_spec = P(("dp", "sp"), None)
    smem = pl.BlockSpec(memory_space=pltpu.SMEM)
    hbm = pl.BlockSpec(memory_space=pltpu.HBM)
    vmem = pl.BlockSpec(memory_space=pltpu.VMEM)
    dma = pltpu.SemaphoreType.DMA

    def local_fn(z_rows, x_rows, v_rows, mask_row, length_scale, out_scale):
        n_src, r_cols = v_rows.shape
        n_tgt, depth = z_rows.shape
        gathered = pl.pallas_call(
            gather_kernel,
            out_shape=[
                jax.ShapeDtypeStruct((2, n_src, depth), BF16),
                jax.ShapeDtypeStruct((2, n_src, 128), BF16),
                jax.ShapeDtypeStruct((2, r_cols, n_src), BF16),
                jax.ShapeDtypeStruct((4, 4, ZROWS, 128), BF16),
                jax.ShapeDtypeStruct((r_cols, n_tgt), F32),
            ],
            in_specs=[smem, smem, hbm, hbm, hbm, hbm],
            out_specs=[vmem] * 5,
            scratch_shapes=[
                pltpu.SMEM(mask_row.shape, jnp.int32),
                pltpu.VMEM((n_tgt, depth), BF16),
                dma((4,)), dma((12,)), dma((12,)), dma((2,)), dma((2,)),
            ],
            compiler_params=pltpu.CompilerParams(
                collective_id=0, has_side_effects=True, vmem_limit_bytes=40 * 2**20),
        )(length_scale, out_scale, *[pltpu.with_memory_space_constraint(a, pltpu.HBM) for a in (mask_row, z_rows, x_rows, v_rows.T)])
        partial = pl.pallas_call(
            block_kernel,
            out_shape=jax.ShapeDtypeStruct((4, r_cols, n_tgt), F32),
            in_specs=[smem, smem] + [vmem] * 5,
            out_specs=vmem,
            scratch_shapes=[pltpu.SMEM((8,), jnp.int32)],
            compiler_params=pltpu.CompilerParams(vmem_limit_bytes=20 * 2**20),
        )(length_scale, out_scale, *gathered)
        y_t = pl.pallas_call(
            sum_kernel,
            out_shape=jax.ShapeDtypeStruct((r_cols, n_tgt), F32),
            in_specs=[smem, smem] + [vmem] * 5,
            out_specs=vmem,
            scratch_shapes=[pltpu.VMEM((3, r_cols, n_tgt), F32), dma((3,)), dma((3,))],
            compiler_params=pltpu.CompilerParams(
                collective_id=1, has_side_effects=True, vmem_limit_bytes=20 * 2**20),
        )(length_scale, out_scale, *gathered[:4], partial)
        return y_t.T

    return jax.shard_map(local_fn, mesh=mesh, in_specs=(row_spec, row_spec, row_spec, row_spec, P(None), P(None)),
                         out_specs=row_spec, check_vma=False)
```

```python
import jax
import jax.numpy as jnp
from jax import lax
from jax.experimental import pallas as pl
from jax.experimental.pallas import tpu as pltpu
from jax.sharding import PartitionSpec as P

F32 = jnp.float32
BF16 = jnp.bfloat16
LOG2E = 1.4426950408889634
PREP = 8192
EARLY = 4096
LATE = 0
TILE = 256
ZROWS = 144
RUN = 3
MESH = pl.DeviceIdType.MESH


def limbs(r):
    first = r.astype(BF16).astype(F32)
    rest = jnp.where(jnp.abs(first) < jnp.inf, r - first, 0.0)
    second = rest.astype(BF16).astype(F32)
    return first, second, rest - second


def scalars(ls_ref, os_ref):
    lv = jnp.full((8, 128), ls_ref[0], F32)
    l2 = lv * lv
    pv = jnp.where(l2 > 2.0**64, 2.0**-64, 1.0)
    l2p = l2 * pv
    return pv, LOG2E / l2p, l2p * jnp.log(jnp.full((8, 128), os_ref[0], F32))


def peer(me, k):
    c = (me % 2 + k % 2) % 2
    x = ((me // 2) % 2 + (k // 2) % 2) % 2
    y = (me // 4 + k // 4) % 2
    return (y * 2 + x) * 2 + c


def piece(z_slot, src, at, rows, c, s, xs, xaug, vs, zall):
    rhs = jnp.concatenate([zall[z_slot, q] for q in range(4)], axis=1)
    lhs = jnp.concatenate([xs[src, at:at + rows, :], xaug[src, at:at + rows, :]], axis=1)[:, :ZROWS]
    t = jnp.dot(lhs, rhs, preferred_element_type=F32)
    kern = jnp.minimum(jnp.exp2(t * c).astype(BF16), s)
    return jnp.dot(vs[src, :, at:at + rows], kern, preferred_element_type=F32)


def mask_bit(zall, slot, dev):
    sub = lax.broadcasted_iota(jnp.int32, (16, 128), 0)
    lane = lax.broadcasted_iota(jnp.int32, (16, 128), 1)
    bits = jnp.where((sub == 6) & (lane == dev), zall[slot, 0, 128:144, :].astype(F32), 0.0)
    return jnp.sum(jnp.sum(bits, axis=0, keepdims=True), axis=1, keepdims=True)


def gather_kernel(ls_ref, os_ref, w_hbm, z_hbm, x_hbm, v_hbm, xs, xaug, vs, zall, own,
                  w_ref, zin, in_sem, zs_sem, zr_sem, xs_sem, xr_sem):
    me = lax.axis_index("sp")
    dp = lax.axis_index("dp")
    zcopy = pltpu.make_async_copy(z_hbm, zin, in_sem.at[0])
    xcopy = pltpu.make_async_copy(x_hbm, xs.at[0], in_sem.at[1])
    vcopy = pltpu.make_async_copy(v_hbm, vs.at[0], in_sem.at[2])
    wcopy = pltpu.make_async_copy(w_hbm, w_ref, in_sem.at[3])
    zcopy.start()
    wcopy.start()
    xcopy.start()
    vcopy.start()
    barrier = pltpu.get_barrier_semaphore()
    for k in (1, 2, 4):
        pl.semaphore_signal(barrier, inc=1, device_id=(dp, peer(me, k)), device_id_type=MESH)

    pv, cvec, lns = scalars(ls_ref, os_ref)
    c = cvec[0, 0]
    s = os_ref[0].astype(BF16)
    sub = lax.broadcasted_iota(jnp.int32, (16, 128), 0)
    lane = lax.broadcasted_iota(jnp.int32, (16, 128), 1)
    wcopy.wait()
    bits = jnp.zeros((16, 128), F32)
    for j in range(8):
        bits = jnp.where(lane == j, w_ref[0, j].astype(F32), bits)
    zcopy.wait()
    for q in range(4):
        zt = zin[pl.ds(128 * q, 128), :].astype(F32).T
        nz = jnp.sum(zt * zt, axis=0, keepdims=True)
        a, b, d = limbs(jnp.broadcast_to(nz, (16, 128)) * (-0.5 * pv[0:1, :]) + lns[0:1, :])
        aug = jnp.where(sub < 3, 1.0, jnp.where(sub == 3, a, jnp.where(sub == 4, b, jnp.where(
            sub == 5, d, jnp.where(sub == 6, bits, 0.0)))))
        zall[0, q, 0:128, :] = (zt * pv[0:1, :]).astype(BF16)
        zall[0, q, 128:144, :] = aug.astype(BF16)

    def zcopy_to(n, src, dst, q, k):
        return pltpu.make_async_remote_copy(
            src_ref=zall.at[src, q], dst_ref=zall.at[dst, q],
            send_sem=zs_sem.at[n], recv_sem=zr_sem.at[n], device_id=(dp, peer(me, k)), device_id_type=MESH)

    order = tuple(zip((0, 1, 2, 3), (2, 3, 0, 1)))
    copies = {name: zcopy_to(n, *name) for n, name in enumerate(
        [one for q, r in order for one in ((0, 1, q, 2), (0, 2, r, 4))]
        + [(1, 3, 0, 4), (2, 3, 2, 2), (1, 3, 1, 4), (2, 3, 3, 2)])}
    xsend = pltpu.make_async_remote_copy(
        src_ref=x_hbm, dst_ref=xs.at[1], send_sem=xs_sem.at[0], recv_sem=xr_sem.at[0],
        device_id=(dp, peer(me, 1)), device_id_type=MESH)
    vsend = pltpu.make_async_remote_copy(
        src_ref=v_hbm, dst_ref=vs.at[1], send_sem=xs_sem.at[1], recv_sem=xr_sem.at[1],
        device_id=(dp, peer(me, 1)), device_id_type=MESH)

    n_src = xs.shape[1]
    ones = jnp.ones((16, 256), BF16)

    def prep(which):
        def body(i, carry):
            r0 = 0
            xf = xs[which, pl.ds(r0, PREP), :].astype(F32)
            sq = xf * xf
            hi = sq.astype(BF16)
            lo = (sq - hi.astype(F32)).astype(BF16)
            nx = lax.dot_general(ones, jnp.concatenate([hi, lo], axis=1), (((1,), (1,)), ((), ())),
                                 preferred_element_type=F32)
            for h in range(PREP // 128):
                a, b, d = limbs(nx[:, 128 * h:128 * h + 128] * (-0.5 * pv[0:1, :]))
                aug = jnp.where(sub == 0, a, jnp.where(sub == 1, b, jnp.where(sub == 2, d, jnp.where(
                    sub < 6, 1.0, 0.0))))
                full = jnp.concatenate([aug.astype(BF16), jnp.zeros((112, 128), BF16)], axis=0)
                xaug[which, pl.ds(r0 + 128 * h, 128), :] = full.T
            return carry
        body(0, 0)

    def pass_on(got, onward):
        copies[got].wait_recv()
        copies[onward].start()

    pl.semaphore_wait(barrier, 3)
    for name in copies:
        if name[0] == 0:
            copies[name].start()
    xsend.start()
    vsend.start()
    xcopy.wait()
    prep(0)
    vcopy.wait()
    first = piece(0, 0, 0, EARLY, c, s, xs, xaug, vs, zall)
    for q in (0, 1):
        pass_on((0, 1, q, 2), (1, 3, q, 4))
        pass_on((0, 2, q + 2, 4), (2, 3, q + 2, 2))
    xsend.wait_recv()
    prep(1)
    own[...] = first + piece(0, 0, EARLY, n_src - EARLY, c, s, xs, xaug, vs, zall)
    vsend.wait_recv()
    if LATE:
        extra = piece(0, 1, 0, LATE, c, s, xs, xaug, vs, zall)
        own[...] += extra * mask_bit(zall, 0, peer(me, 1))
    for q, r in order[2:]:
        copies[(0, 1, q, 2)].wait_recv()
        copies[(0, 2, r, 4)].wait_recv()
    for name in ((1, 3, 0, 4), (2, 3, 2, 2), (1, 3, 1, 4), (2, 3, 3, 2)):
        copies[name].wait_recv()
    for copy in (*copies.values(), xsend, vsend):
        copy.wait_send()


def block_kernel(ls_ref, os_ref, xs, xaug, vs, zall, own, y_ref, pairs):
    me = lax.axis_index("sp")
    _, cvec, _ = scalars(ls_ref, os_ref)
    c = cvec[0, 0]
    s = os_ref[0].astype(BF16)
    n_tiles = xs.shape[1] // TILE
    count = jnp.int32(0)
    for e in range(2, 8):
        pairs[count] = jnp.int32(e)
        count += mask_bit(zall, e // 2, peer(me, e % 2))[0, 0].astype(jnp.int32)
    y_ref[0] = own[...]
    for slot in range(1, 4):
        y_ref[slot] = jnp.zeros_like(own)

    def main(*accs):
        g_acc = (accs[0:3], accs[3:6])
        y_acc = (accs[6:8], accs[8:10])
        zero_rows = jnp.zeros((256 - ZROWS, 256), BF16)

        def run(start, n):
            slots = [pairs[start + i] // 2 for i in range(n)]
            srcs = [pairs[start + i] % 2 for i in range(n)]
            tiles = [(i, j) for i in range(n) for j in range(n_tiles)]

            def first(g):
                i, j = tiles[g]
                for m in range(2):
                    rows = jnp.concatenate([zall[slots[i], 2 * m], zall[slots[i], 2 * m + 1]], axis=1)
                    pltpu.matmul_push_rhs(jnp.concatenate([rows, zero_rows], axis=0), staging_register=0, mxu_index=m)
                at = pl.ds(j * TILE, TILE)
                lhs = jnp.concatenate([xs[srcs[i], at, :], xaug[srcs[i], at, :]], axis=1)
                for m in range(2):
                    pltpu.matmul_acc_lhs(g_acc[m][g % 3], lhs, load_staged_rhs=0)

            def second(g):
                i, j = tiles[g]
                for m in range(2):
                    t = pltpu.matmul_pop(g_acc[m][g % 3])
                    kern = jnp.minimum(jnp.exp2(t * c).astype(BF16), s)
                    pltpu.matmul_push_rhs(kern, staging_register=1, mxu_index=m)
                for m in range(2):
                    pltpu.matmul_acc_lhs(y_acc[i % 2][m], vs[srcs[i], :, pl.ds(j * TILE, TILE)], load_staged_rhs=1)

            def finish(i):
                for m in range(2):
                    y_ref[slots[i], :, 256 * m:256 * m + 256] += pltpu.matmul_pop(y_acc[i % 2][m])

            for g in range(len(tiles)):
                first(g)
                if g >= 2:
                    second(g - 2)
                if g > n_tiles and g % n_tiles == 6:
                    finish(g // n_tiles - 1)
            second(len(tiles) - 2)
            second(len(tiles) - 1)
            finish(n - 1)

        def full(i, carry):
            run(i * RUN, RUN)
            return carry

        lax.fori_loop(0, count // RUN, full, 0)
        for n in range(1, RUN):
            @pl.when(count % RUN == n)
            def _():
                run(count - n, n)

    big = [pltpu.ACC(m)((TILE, 256), F32) for m in (0, 0, 0, 1, 1, 1)]
    small = [pltpu.ACC(m)((16, 256), F32) for m in (0, 1, 0, 1)]
    pl.run_scoped(main, *big, *small)


def sum_kernel(ls_ref, os_ref, xs, xaug, vs, zall, y_ref, o_ref, yrecv, s_sem, r_sem):
    me = lax.axis_index("sp")
    dp = lax.axis_index("dp")
    barrier = pltpu.get_barrier_semaphore()
    for k in (2, 4, 6):
        pl.semaphore_signal(barrier, inc=1, device_id=(dp, peer(me, k)), device_id_type=MESH)
    pl.semaphore_wait(barrier, 3)
    copies = [pltpu.make_async_remote_copy(
        src_ref=y_ref.at[n + 1], dst_ref=yrecv.at[n], send_sem=s_sem.at[n], recv_sem=r_sem.at[n],
        device_id=(dp, peer(me, 2 * n + 2)), device_id_type=MESH) for n in (2, 0, 1)]
    for copy in copies:
        copy.start()
    _, cvec, _ = scalars(ls_ref, os_ref)
    rest = piece(0, 1, LATE, xs.shape[1] - LATE, cvec[0, 0], os_ref[0].astype(BF16), xs, xaug, vs, zall)
    own = y_ref[0] + rest * mask_bit(zall, 0, peer(me, 1))
    for copy in copies:
        copy.wait_recv()
    o_ref[...] = (own + yrecv[0]) + (yrecv[1] + yrecv[2])
    for copy in copies:
        copy.wait_send()


def solution(mesh):
    row_spec = P(("dp", "sp"), None)
    smem = pl.BlockSpec(memory_space=pltpu.SMEM)
    hbm = pl.BlockSpec(memory_space=pltpu.HBM)
    vmem = pl.BlockSpec(memory_space=pltpu.VMEM)
    dma = pltpu.SemaphoreType.DMA

    def local_fn(z_rows, x_rows, v_rows, mask_row, length_scale, out_scale):
        n_src, r_cols = v_rows.shape
        n_tgt, depth = z_rows.shape
        gathered = pl.pallas_call(
            gather_kernel,
            out_shape=[
                jax.ShapeDtypeStruct((2, n_src, depth), BF16),
                jax.ShapeDtypeStruct((2, n_src, 128), BF16),
                jax.ShapeDtypeStruct((2, r_cols, n_src), BF16),
                jax.ShapeDtypeStruct((4, 4, ZROWS, 128), BF16),
                jax.ShapeDtypeStruct((r_cols, n_tgt), F32),
            ],
            in_specs=[smem, smem, hbm, hbm, hbm, hbm],
            out_specs=[vmem] * 5,
            scratch_shapes=[
                pltpu.SMEM(mask_row.shape, jnp.int32),
                pltpu.VMEM((n_tgt, depth), BF16),
                dma((4,)), dma((12,)), dma((12,)), dma((2,)), dma((2,)),
            ],
            compiler_params=pltpu.CompilerParams(
                collective_id=0, has_side_effects=True, vmem_limit_bytes=40 * 2**20),
        )(length_scale, out_scale, *[pltpu.with_memory_space_constraint(a, pltpu.HBM) for a in (mask_row, z_rows, x_rows, v_rows.T)])
        partial = pl.pallas_call(
            block_kernel,
            out_shape=jax.ShapeDtypeStruct((4, r_cols, n_tgt), F32),
            in_specs=[smem, smem] + [vmem] * 5,
            out_specs=vmem,
            scratch_shapes=[pltpu.SMEM((8,), jnp.int32)],
            compiler_params=pltpu.CompilerParams(vmem_limit_bytes=20 * 2**20),
        )(length_scale, out_scale, *gathered)
        y_t = pl.pallas_call(
            sum_kernel,
            out_shape=jax.ShapeDtypeStruct((r_cols, n_tgt), F32),
            in_specs=[smem, smem] + [vmem] * 5,
            out_specs=vmem,
            scratch_shapes=[pltpu.VMEM((3, r_cols, n_tgt), F32), dma((3,)), dma((3,))],
            compiler_params=pltpu.CompilerParams(
                collective_id=1, has_side_effects=True, vmem_limit_bytes=20 * 2**20),
        )(length_scale, out_scale, *gathered[:4], partial)
        return y_t.T

    return jax.shard_map(local_fn, mesh=mesh, in_specs=(row_spec, row_spec, row_spec, row_spec, P(None), P(None)),
                         out_specs=row_spec, check_vma=False)
```

```python
import jax
import jax.numpy as jnp
from jax import lax
from jax.experimental import pallas as pl
from jax.experimental.pallas import tpu as pltpu
from jax.sharding import PartitionSpec as P

F32 = jnp.float32
BF16 = jnp.bfloat16
LOG2E = 1.4426950408889634
PREP = 8192
EARLY = 6144
LATE = 0
TILE = 256
ZROWS = 144
RUN = 3
MESH = pl.DeviceIdType.MESH


def limbs(r):
    first = r.astype(BF16).astype(F32)
    rest = jnp.where(jnp.abs(first) < jnp.inf, r - first, 0.0)
    second = rest.astype(BF16).astype(F32)
    return first, second, rest - second


def scalars(ls_ref, os_ref):
    lv = jnp.full((8, 128), ls_ref[0], F32)
    l2 = lv * lv
    pv = jnp.where(l2 > 2.0**64, 2.0**-64, 1.0)
    l2p = l2 * pv
    return pv, LOG2E / l2p, l2p * jnp.log(jnp.full((8, 128), os_ref[0], F32))


def peer(me, k):
    c = (me % 2 + k % 2) % 2
    x = ((me // 2) % 2 + (k // 2) % 2) % 2
    y = (me // 4 + k // 4) % 2
    return (y * 2 + x) * 2 + c


def piece(z_slot, src, at, rows, c, s, xs, xaug, vs, zall):
    rhs = jnp.concatenate([zall[z_slot, q] for q in range(4)], axis=1)
    lhs = jnp.concatenate([xs[src, at:at + rows, :], xaug[src, at:at + rows, :]], axis=1)[:, :ZROWS]
    t = jnp.dot(lhs, rhs, preferred_element_type=F32)
    kern = jnp.minimum(jnp.exp2(t * c).astype(BF16), s)
    return jnp.dot(vs[src, :, at:at + rows], kern, preferred_element_type=F32)


def mask_bit(zall, slot, dev):
    sub = lax.broadcasted_iota(jnp.int32, (16, 128), 0)
    lane = lax.broadcasted_iota(jnp.int32, (16, 128), 1)
    bits = jnp.where((sub == 6) & (lane == dev), zall[slot, 0, 128:144, :].astype(F32), 0.0)
    return jnp.sum(jnp.sum(bits, axis=0, keepdims=True), axis=1, keepdims=True)


def gather_kernel(ls_ref, os_ref, w_hbm, z_hbm, x_hbm, v_hbm, xs, xaug, vs, zall, own,
                  w_ref, zin, in_sem, zs_sem, zr_sem, xs_sem, xr_sem):
    me = lax.axis_index("sp")
    dp = lax.axis_index("dp")
    zcopy = pltpu.make_async_copy(z_hbm, zin, in_sem.at[0])
    xcopy = pltpu.make_async_copy(x_hbm, xs.at[0], in_sem.at[1])
    vcopy = pltpu.make_async_copy(v_hbm, vs.at[0], in_sem.at[2])
    wcopy = pltpu.make_async_copy(w_hbm, w_ref, in_sem.at[3])
    zcopy.start()
    wcopy.start()
    xcopy.start()
    vcopy.start()
    barrier = pltpu.get_barrier_semaphore()
    for k in (1, 2, 4):
        pl.semaphore_signal(barrier, inc=1, device_id=(dp, peer(me, k)), device_id_type=MESH)

    pv, cvec, lns = scalars(ls_ref, os_ref)
    c = cvec[0, 0]
    s = os_ref[0].astype(BF16)
    sub = lax.broadcasted_iota(jnp.int32, (16, 128), 0)
    lane = lax.broadcasted_iota(jnp.int32, (16, 128), 1)
    wcopy.wait()
    bits = jnp.zeros((16, 128), F32)
    for j in range(8):
        bits = jnp.where(lane == j, w_ref[0, j].astype(F32), bits)
    zcopy.wait()
    for q in range(4):
        zt = zin[pl.ds(128 * q, 128), :].astype(F32).T
        nz = jnp.sum(zt * zt, axis=0, keepdims=True)
        a, b, d = limbs(jnp.broadcast_to(nz, (16, 128)) * (-0.5 * pv[0:1, :]) + lns[0:1, :])
        aug = jnp.where(sub < 3, 1.0, jnp.where(sub == 3, a, jnp.where(sub == 4, b, jnp.where(
            sub == 5, d, jnp.where(sub == 6, bits, 0.0)))))
        zall[0, q, 0:128, :] = (zt * pv[0:1, :]).astype(BF16)
        zall[0, q, 128:144, :] = aug.astype(BF16)

    def zcopy_to(n, src, dst, q, k):
        return pltpu.make_async_remote_copy(
            src_ref=zall.at[src, q], dst_ref=zall.at[dst, q],
            send_sem=zs_sem.at[n], recv_sem=zr_sem.at[n], device_id=(dp, peer(me, k)), device_id_type=MESH)

    order = tuple(zip((0, 1, 2, 3), (2, 3, 0, 1)))
    copies = {name: zcopy_to(n, *name) for n, name in enumerate(
        [one for q, r in order for one in ((0, 1, q, 2), (0, 2, r, 4))]
        + [(1, 3, 0, 4), (2, 3, 2, 2), (1, 3, 1, 4), (2, 3, 3, 2)])}
    xsend = pltpu.make_async_remote_copy(
        src_ref=x_hbm, dst_ref=xs.at[1], send_sem=xs_sem.at[0], recv_sem=xr_sem.at[0],
        device_id=(dp, peer(me, 1)), device_id_type=MESH)
    vsend = pltpu.make_async_remote_copy(
        src_ref=v_hbm, dst_ref=vs.at[1], send_sem=xs_sem.at[1], recv_sem=xr_sem.at[1],
        device_id=(dp, peer(me, 1)), device_id_type=MESH)

    n_src = xs.shape[1]
    ones = jnp.ones((16, 256), BF16)

    def prep(which):
        def body(i, carry):
            r0 = 0
            xf = xs[which, pl.ds(r0, PREP), :].astype(F32)
            sq = xf * xf
            hi = sq.astype(BF16)
            lo = (sq - hi.astype(F32)).astype(BF16)
            nx = lax.dot_general(ones, jnp.concatenate([hi, lo], axis=1), (((1,), (1,)), ((), ())),
                                 preferred_element_type=F32)
            for h in range(PREP // 128):
                a, b, d = limbs(nx[:, 128 * h:128 * h + 128] * (-0.5 * pv[0:1, :]))
                aug = jnp.where(sub == 0, a, jnp.where(sub == 1, b, jnp.where(sub == 2, d, jnp.where(
                    sub < 6, 1.0, 0.0))))
                full = jnp.concatenate([aug.astype(BF16), jnp.zeros((112, 128), BF16)], axis=0)
                xaug[which, pl.ds(r0 + 128 * h, 128), :] = full.T
            return carry
        body(0, 0)

    def pass_on(got, onward):
        copies[got].wait_recv()
        copies[onward].start()

    pl.semaphore_wait(barrier, 3)
    for name in copies:
        if name[0] == 0:
            copies[name].start()
    xsend.start()
    vsend.start()
    xcopy.wait()
    prep(0)
    vcopy.wait()
    first = piece(0, 0, 0, EARLY, c, s, xs, xaug, vs, zall)
    for q in (0, 1):
        pass_on((0, 1, q, 2), (1, 3, q, 4))
        pass_on((0, 2, q + 2, 4), (2, 3, q + 2, 2))
    xsend.wait_recv()
    prep(1)
    own[...] = first + piece(0, 0, EARLY, n_src - EARLY, c, s, xs, xaug, vs, zall)
    vsend.wait_recv()
    if LATE:
        extra = piece(0, 1, 0, LATE, c, s, xs, xaug, vs, zall)
        own[...] += extra * mask_bit(zall, 0, peer(me, 1))
    for q, r in order[2:]:
        copies[(0, 1, q, 2)].wait_recv()
        copies[(0, 2, r, 4)].wait_recv()
    for name in ((1, 3, 0, 4), (2, 3, 2, 2), (1, 3, 1, 4), (2, 3, 3, 2)):
        copies[name].wait_recv()
    for copy in (*copies.values(), xsend, vsend):
        copy.wait_send()


def block_kernel(ls_ref, os_ref, xs, xaug, vs, zall, own, y_ref, pairs):
    me = lax.axis_index("sp")
    _, cvec, _ = scalars(ls_ref, os_ref)
    c = cvec[0, 0]
    s = os_ref[0].astype(BF16)
    n_tiles = xs.shape[1] // TILE
    count = jnp.int32(0)
    for e in range(2, 8):
        pairs[count] = jnp.int32(e)
        count += mask_bit(zall, e // 2, peer(me, e % 2))[0, 0].astype(jnp.int32)
    y_ref[0] = own[...]
    for slot in range(1, 4):
        y_ref[slot] = jnp.zeros_like(own)

    def main(*accs):
        g_acc = (accs[0:3], accs[3:6])
        y_acc = (accs[6:8], accs[8:10])
        zero_rows = jnp.zeros((256 - ZROWS, 256), BF16)

        def run(start, n):
            slots = [pairs[start + i] // 2 for i in range(n)]
            srcs = [pairs[start + i] % 2 for i in range(n)]
            tiles = [(i, j) for i in range(n) for j in range(n_tiles)]

            def first(g):
                i, j = tiles[g]
                for m in range(2):
                    rows = jnp.concatenate([zall[slots[i], 2 * m], zall[slots[i], 2 * m + 1]], axis=1)
                    pltpu.matmul_push_rhs(jnp.concatenate([rows, zero_rows], axis=0), staging_register=0, mxu_index=m)
                at = pl.ds(j * TILE, TILE)
                lhs = jnp.concatenate([xs[srcs[i], at, :], xaug[srcs[i], at, :]], axis=1)
                for m in range(2):
                    pltpu.matmul_acc_lhs(g_acc[m][g % 3], lhs, load_staged_rhs=0)

            def second(g):
                i, j = tiles[g]
                for m in range(2):
                    t = pltpu.matmul_pop(g_acc[m][g % 3])
                    kern = jnp.minimum(jnp.exp2(t * c).astype(BF16), s)
                    pltpu.matmul_push_rhs(kern, staging_register=1, mxu_index=m)
                for m in range(2):
                    pltpu.matmul_acc_lhs(y_acc[i % 2][m], vs[srcs[i], :, pl.ds(j * TILE, TILE)], load_staged_rhs=1)

            def finish(i):
                for m in range(2):
                    y_ref[slots[i], :, 256 * m:256 * m + 256] += pltpu.matmul_pop(y_acc[i % 2][m])

            for g in range(len(tiles)):
                first(g)
                if g >= 2:
                    second(g - 2)
                if g > n_tiles and g % n_tiles == 6:
                    finish(g // n_tiles - 1)
            second(len(tiles) - 2)
            second(len(tiles) - 1)
            finish(n - 1)

        def full(i, carry):
            run(i * RUN, RUN)
            return carry

        lax.fori_loop(0, count // RUN, full, 0)
        for n in range(1, RUN):
            @pl.when(count % RUN == n)
            def _():
                run(count - n, n)

    big = [pltpu.ACC(m)((TILE, 256), F32) for m in (0, 0, 0, 1, 1, 1)]
    small = [pltpu.ACC(m)((16, 256), F32) for m in (0, 1, 0, 1)]
    pl.run_scoped(main, *big, *small)


def sum_kernel(ls_ref, os_ref, xs, xaug, vs, zall, y_ref, o_ref, yrecv, s_sem, r_sem):
    me = lax.axis_index("sp")
    dp = lax.axis_index("dp")
    barrier = pltpu.get_barrier_semaphore()
    for k in (2, 4, 6):
        pl.semaphore_signal(barrier, inc=1, device_id=(dp, peer(me, k)), device_id_type=MESH)
    pl.semaphore_wait(barrier, 3)
    copies = [pltpu.make_async_remote_copy(
        src_ref=y_ref.at[n + 1], dst_ref=yrecv.at[n], send_sem=s_sem.at[n], recv_sem=r_sem.at[n],
        device_id=(dp, peer(me, 2 * n + 2)), device_id_type=MESH) for n in (2, 0, 1)]
    for copy in copies:
        copy.start()
    _, cvec, _ = scalars(ls_ref, os_ref)
    rest = piece(0, 1, LATE, xs.shape[1] - LATE, cvec[0, 0], os_ref[0].astype(BF16), xs, xaug, vs, zall)
    own = y_ref[0] + rest * mask_bit(zall, 0, peer(me, 1))
    for copy in copies:
        copy.wait_recv()
    o_ref[...] = (own + yrecv[0]) + (yrecv[1] + yrecv[2])
    for copy in copies:
        copy.wait_send()


def solution(mesh):
    row_spec = P(("dp", "sp"), None)
    smem = pl.BlockSpec(memory_space=pltpu.SMEM)
    hbm = pl.BlockSpec(memory_space=pltpu.HBM)
    vmem = pl.BlockSpec(memory_space=pltpu.VMEM)
    dma = pltpu.SemaphoreType.DMA

    def local_fn(z_rows, x_rows, v_rows, mask_row, length_scale, out_scale):
        n_src, r_cols = v_rows.shape
        n_tgt, depth = z_rows.shape
        gathered = pl.pallas_call(
            gather_kernel,
            out_shape=[
                jax.ShapeDtypeStruct((2, n_src, depth), BF16),
                jax.ShapeDtypeStruct((2, n_src, 128), BF16),
                jax.ShapeDtypeStruct((2, r_cols, n_src), BF16),
                jax.ShapeDtypeStruct((4, 4, ZROWS, 128), BF16),
                jax.ShapeDtypeStruct((r_cols, n_tgt), F32),
            ],
            in_specs=[smem, smem, hbm, hbm, hbm, hbm],
            out_specs=[vmem] * 5,
            scratch_shapes=[
                pltpu.SMEM(mask_row.shape, jnp.int32),
                pltpu.VMEM((n_tgt, depth), BF16),
                dma((4,)), dma((12,)), dma((12,)), dma((2,)), dma((2,)),
            ],
            compiler_params=pltpu.CompilerParams(
                collective_id=0, has_side_effects=True, vmem_limit_bytes=40 * 2**20),
        )(length_scale, out_scale, *[pltpu.with_memory_space_constraint(a, pltpu.HBM) for a in (mask_row, z_rows, x_rows, v_rows.T)])
        partial = pl.pallas_call(
            block_kernel,
            out_shape=jax.ShapeDtypeStruct((4, r_cols, n_tgt), F32),
            in_specs=[smem, smem] + [vmem] * 5,
            out_specs=vmem,
            scratch_shapes=[pltpu.SMEM((8,), jnp.int32)],
            compiler_params=pltpu.CompilerParams(vmem_limit_bytes=20 * 2**20),
        )(length_scale, out_scale, *gathered)
        y_t = pl.pallas_call(
            sum_kernel,
            out_shape=jax.ShapeDtypeStruct((r_cols, n_tgt), F32),
            in_specs=[smem, smem] + [vmem] * 5,
            out_specs=vmem,
            scratch_shapes=[pltpu.VMEM((3, r_cols, n_tgt), F32), dma((3,)), dma((3,))],
            compiler_params=pltpu.CompilerParams(
                collective_id=1, has_side_effects=True, vmem_limit_bytes=20 * 2**20),
        )(length_scale, out_scale, *gathered[:4], partial)
        return y_t.T

    return jax.shard_map(local_fn, mesh=mesh, in_specs=(row_spec, row_spec, row_spec, row_spec, P(None), P(None)),
                         out_specs=row_spec, check_vma=False)
```

```python
import jax
import jax.numpy as jnp
from jax import lax
from jax.experimental import pallas as pl
from jax.experimental.pallas import tpu as pltpu
from jax.sharding import PartitionSpec as P

F32 = jnp.float32
BF16 = jnp.bfloat16
LOG2E = 1.4426950408889634
PREP = 8192
EARLY = 6144
LATE = 0
TILE = 256
ZROWS = 144
RUN = 3
MESH = pl.DeviceIdType.MESH


def limbs(r):
    first = r.astype(BF16).astype(F32)
    rest = jnp.where(jnp.abs(first) < jnp.inf, r - first, 0.0)
    second = rest.astype(BF16).astype(F32)
    return first, second, rest - second


def scalars(ls_ref, os_ref):
    lv = jnp.full((8, 128), ls_ref[0], F32)
    l2 = lv * lv
    pv = jnp.where(l2 > 2.0**64, 2.0**-64, 1.0)
    l2p = l2 * pv
    return pv, LOG2E / l2p, l2p * jnp.log(jnp.full((8, 128), os_ref[0], F32))


def peer(me, k):
    c = (me % 2 + k % 2) % 2
    x = ((me // 2) % 2 + (k // 2) % 2) % 2
    y = (me // 4 + k // 4) % 2
    return (y * 2 + x) * 2 + c


def piece(z_slot, src, at, rows, c, s, xs, xaug, vs, zall):
    rhs = jnp.concatenate([zall[z_slot, q] for q in range(4)], axis=1)
    lhs = jnp.concatenate([xs[src, at:at + rows, :], xaug[src, at:at + rows, :]], axis=1)[:, :ZROWS]
    t = jnp.dot(lhs, rhs, preferred_element_type=F32)
    kern = jnp.minimum(jnp.exp2(t * c).astype(BF16), s)
    return jnp.dot(vs[src, :, at:at + rows], kern, preferred_element_type=F32)


def mask_bit(zall, slot, dev):
    sub = lax.broadcasted_iota(jnp.int32, (16, 128), 0)
    lane = lax.broadcasted_iota(jnp.int32, (16, 128), 1)
    bits = jnp.where((sub == 6) & (lane == dev), zall[slot, 0, 128:144, :].astype(F32), 0.0)
    return jnp.sum(jnp.sum(bits, axis=0, keepdims=True), axis=1, keepdims=True)


def gather_kernel(ls_ref, os_ref, w_hbm, z_hbm, x_hbm, v_hbm, xs, xaug, vs, zall, own,
                  w_ref, zin, in_sem, zs_sem, zr_sem, xs_sem, xr_sem):
    me = lax.axis_index("sp")
    dp = lax.axis_index("dp")
    zcopy = pltpu.make_async_copy(z_hbm, zin, in_sem.at[0])
    xcopy = pltpu.make_async_copy(x_hbm, xs.at[0], in_sem.at[1])
    vcopy = pltpu.make_async_copy(v_hbm, vs.at[0], in_sem.at[2])
    wcopy = pltpu.make_async_copy(w_hbm, w_ref, in_sem.at[3])
    zcopy.start()
    wcopy.start()
    xcopy.start()
    vcopy.start()
    barrier = pltpu.get_barrier_semaphore()
    for k in (1, 2, 4):
        pl.semaphore_signal(barrier, inc=1, device_id=(dp, peer(me, k)), device_id_type=MESH)

    pv, cvec, lns = scalars(ls_ref, os_ref)
    c = cvec[0, 0]
    s = os_ref[0].astype(BF16)
    sub = lax.broadcasted_iota(jnp.int32, (16, 128), 0)
    lane = lax.broadcasted_iota(jnp.int32, (16, 128), 1)
    wcopy.wait()
    bits = jnp.zeros((16, 128), F32)
    for j in range(8):
        bits = jnp.where(lane == j, w_ref[0, j].astype(F32), bits)
    zcopy.wait()
    for q in range(4):
        zt = zin[pl.ds(128 * q, 128), :].astype(F32).T
        nz = jnp.sum(zt * zt, axis=0, keepdims=True)
        a, b, d = limbs(jnp.broadcast_to(nz, (16, 128)) * (-0.5 * pv[0:1, :]) + lns[0:1, :])
        aug = jnp.where(sub < 3, 1.0, jnp.where(sub == 3, a, jnp.where(sub == 4, b, jnp.where(
            sub == 5, d, jnp.where(sub == 6, bits, 0.0)))))
        zall[0, q, 0:128, :] = (zt * pv[0:1, :]).astype(BF16)
        zall[0, q, 128:144, :] = aug.astype(BF16)

    def zcopy_to(n, src, dst, q, k):
        return pltpu.make_async_remote_copy(
            src_ref=zall.at[src, q], dst_ref=zall.at[dst, q],
            send_sem=zs_sem.at[n], recv_sem=zr_sem.at[n], device_id=(dp, peer(me, k)), device_id_type=MESH)

    order = tuple(zip((0, 1, 2, 3), (2, 3, 0, 1)))
    copies = {name: zcopy_to(n, *name) for n, name in enumerate(
        [one for q, r in order for one in ((0, 1, q, 2), (0, 2, r, 4))]
        + [(1, 3, 0, 4), (2, 3, 2, 2), (1, 3, 1, 4), (2, 3, 3, 2)])}
    xsend = pltpu.make_async_remote_copy(
        src_ref=x_hbm, dst_ref=xs.at[1], send_sem=xs_sem.at[0], recv_sem=xr_sem.at[0],
        device_id=(dp, peer(me, 1)), device_id_type=MESH)
    vsend = pltpu.make_async_remote_copy(
        src_ref=v_hbm, dst_ref=vs.at[1], send_sem=xs_sem.at[1], recv_sem=xr_sem.at[1],
        device_id=(dp, peer(me, 1)), device_id_type=MESH)

    n_src = xs.shape[1]
    ones = jnp.ones((16, 256), BF16)

    def prep(which):
        def body(i, carry):
            r0 = 0
            xf = xs[which, pl.ds(r0, PREP), :].astype(F32)
            sq = xf * xf
            hi = sq.astype(BF16)
            lo = (sq - hi.astype(F32)).astype(BF16)
            nx = lax.dot_general(ones, jnp.concatenate([hi, lo], axis=1), (((1,), (1,)), ((), ())),
                                 preferred_element_type=F32)
            for h in range(PREP // 128):
                a, b, d = limbs(nx[:, 128 * h:128 * h + 128] * (-0.5 * pv[0:1, :]))
                aug = jnp.where(sub == 0, a, jnp.where(sub == 1, b, jnp.where(sub == 2, d, jnp.where(
                    sub < 6, 1.0, 0.0))))
                full = jnp.concatenate([aug.astype(BF16), jnp.zeros((112, 128), BF16)], axis=0)
                xaug[which, pl.ds(r0 + 128 * h, 128), :] = full.T
            return carry
        body(0, 0)

    def pass_on(got, onward):
        copies[got].wait_recv()
        copies[onward].start()

    pl.semaphore_wait(barrier, 3)
    for name in copies:
        if name[0] == 0:
            copies[name].start()
    xsend.start()
    vsend.start()
    xcopy.wait()
    prep(0)
    vcopy.wait()
    first = piece(0, 0, 0, EARLY, c, s, xs, xaug, vs, zall)
    for q in (0, 1):
        pass_on((0, 1, q, 2), (1, 3, q, 4))
        pass_on((0, 2, q + 2, 4), (2, 3, q + 2, 2))
    xsend.wait_recv()
    prep(1)
    own[...] = first + piece(0, 0, EARLY, n_src - EARLY, c, s, xs, xaug, vs, zall)
    vsend.wait_recv()
    if LATE:
        extra = piece(0, 1, 0, LATE, c, s, xs, xaug, vs, zall)
        own[...] += extra * mask_bit(zall, 0, peer(me, 1))
    for q, r in order[2:]:
        copies[(0, 1, q, 2)].wait_recv()
        copies[(0, 2, r, 4)].wait_recv()
    for name in ((1, 3, 0, 4), (2, 3, 2, 2), (1, 3, 1, 4), (2, 3, 3, 2)):
        copies[name].wait_recv()
    for copy in (*copies.values(), xsend, vsend):
        copy.wait_send()


def block_kernel(ls_ref, os_ref, xs, xaug, vs, zall, own, y_ref, pairs):
    me = lax.axis_index("sp")
    _, cvec, _ = scalars(ls_ref, os_ref)
    c = cvec[0, 0]
    s = os_ref[0].astype(BF16)
    n_tiles = xs.shape[1] // TILE
    sub = lax.broadcasted_iota(jnp.int32, (16, 128), 0)
    lane = lax.broadcasted_iota(jnp.int32, (16, 128), 1)
    total = jnp.zeros((16, 128), F32)
    for e in range(2, 8):
        hit = (sub == 6) & (lane == peer(me, e % 2))
        total += jnp.where(hit, zall[e // 2, 0, 128:144, :].astype(F32) * 2.0**e, 0.0)
    code = jnp.sum(total).astype(jnp.int32)
    count = jnp.int32(0)
    for e in range(2, 8):
        pairs[count] = jnp.int32(e)
        count += (code >> e) & 1
    y_ref[0] = own[...]
    for slot in range(1, 4):
        y_ref[slot] = jnp.zeros_like(own)

    def main(*accs):
        g_acc = (accs[0:3], accs[3:6])
        y_acc = (accs[6:8], accs[8:10])
        zero_rows = jnp.zeros((256 - ZROWS, 256), BF16)

        def run(start, n):
            slots = [pairs[start + i] // 2 for i in range(n)]
            srcs = [pairs[start + i] % 2 for i in range(n)]
            tiles = [(i, j) for i in range(n) for j in range(n_tiles)]

            def first(g):
                i, j = tiles[g]
                for m in range(2):
                    rows = jnp.concatenate([zall[slots[i], 2 * m], zall[slots[i], 2 * m + 1]], axis=1)
                    pltpu.matmul_push_rhs(jnp.concatenate([rows, zero_rows], axis=0), staging_register=0, mxu_index=m)
                at = pl.ds(j * TILE, TILE)
                lhs = jnp.concatenate([xs[srcs[i], at, :], xaug[srcs[i], at, :]], axis=1)
                for m in range(2):
                    pltpu.matmul_acc_lhs(g_acc[m][g % 3], lhs, load_staged_rhs=0)

            def second(g):
                i, j = tiles[g]
                for m in range(2):
                    t = pltpu.matmul_pop(g_acc[m][g % 3])
                    kern = jnp.minimum(jnp.exp2(t * c).astype(BF16), s)
                    pltpu.matmul_push_rhs(kern, staging_register=1, mxu_index=m)
                for m in range(2):
                    pltpu.matmul_acc_lhs(y_acc[i % 2][m], vs[srcs[i], :, pl.ds(j * TILE, TILE)], load_staged_rhs=1)

            def finish(i):
                for m in range(2):
                    y_ref[slots[i], :, 256 * m:256 * m + 256] += pltpu.matmul_pop(y_acc[i % 2][m])

            for g in range(len(tiles)):
                first(g)
                if g >= 2:
                    second(g - 2)
                if g > n_tiles and g % n_tiles == 6:
                    finish(g // n_tiles - 1)
            second(len(tiles) - 2)
            second(len(tiles) - 1)
            finish(n - 1)

        def full(i, carry):
            run(i * RUN, RUN)
            return carry

        for n in range(1, RUN):
            @pl.when(count % RUN == n)
            def _():
                run(count - n, n)

        lax.fori_loop(0, count // RUN, full, 0)

    big = [pltpu.ACC(m)((TILE, 256), F32) for m in (0, 0, 0, 1, 1, 1)]
    small = [pltpu.ACC(m)((16, 256), F32) for m in (0, 1, 0, 1)]
    pl.run_scoped(main, *big, *small)


def sum_kernel(ls_ref, os_ref, xs, xaug, vs, zall, y_ref, o_ref, yrecv, s_sem, r_sem):
    me = lax.axis_index("sp")
    dp = lax.axis_index("dp")
    barrier = pltpu.get_barrier_semaphore()
    for k in (2, 4, 6):
        pl.semaphore_signal(barrier, inc=1, device_id=(dp, peer(me, k)), device_id_type=MESH)
    pl.semaphore_wait(barrier, 3)
    copies = [pltpu.make_async_remote_copy(
        src_ref=y_ref.at[n + 1], dst_ref=yrecv.at[n], send_sem=s_sem.at[n], recv_sem=r_sem.at[n],
        device_id=(dp, peer(me, 2 * n + 2)), device_id_type=MESH) for n in (2, 0, 1)]
    for copy in copies:
        copy.start()
    _, cvec, _ = scalars(ls_ref, os_ref)
    half = xs.shape[1] // 2
    rest = sum(piece(0, 1, at, half, cvec[0, 0], os_ref[0].astype(BF16), xs, xaug, vs, zall) for at in (0, half))
    own = y_ref[0] + rest * mask_bit(zall, 0, peer(me, 1))
    for copy in copies:
        copy.wait_recv()
    o_ref[...] = (own + yrecv[0]) + (yrecv[1] + yrecv[2])
    for copy in copies:
        copy.wait_send()


def solution(mesh):
    row_spec = P(("dp", "sp"), None)
    smem = pl.BlockSpec(memory_space=pltpu.SMEM)
    hbm = pl.BlockSpec(memory_space=pltpu.HBM)
    vmem = pl.BlockSpec(memory_space=pltpu.VMEM)
    dma = pltpu.SemaphoreType.DMA

    def local_fn(z_rows, x_rows, v_rows, mask_row, length_scale, out_scale):
        n_src, r_cols = v_rows.shape
        n_tgt, depth = z_rows.shape
        gathered = pl.pallas_call(
            gather_kernel,
            out_shape=[
                jax.ShapeDtypeStruct((2, n_src, depth), BF16),
                jax.ShapeDtypeStruct((2, n_src, 128), BF16),
                jax.ShapeDtypeStruct((2, r_cols, n_src), BF16),
                jax.ShapeDtypeStruct((4, 4, ZROWS, 128), BF16),
                jax.ShapeDtypeStruct((r_cols, n_tgt), F32),
            ],
            in_specs=[smem, smem, hbm, hbm, hbm, hbm],
            out_specs=[vmem] * 5,
            scratch_shapes=[
                pltpu.SMEM(mask_row.shape, jnp.int32),
                pltpu.VMEM((n_tgt, depth), BF16),
                dma((4,)), dma((12,)), dma((12,)), dma((2,)), dma((2,)),
            ],
            compiler_params=pltpu.CompilerParams(
                collective_id=0, has_side_effects=True, vmem_limit_bytes=40 * 2**20),
        )(length_scale, out_scale, *[pltpu.with_memory_space_constraint(a, pltpu.HBM) for a in (mask_row, z_rows, x_rows, v_rows.T)])
        partial = pl.pallas_call(
            block_kernel,
            out_shape=jax.ShapeDtypeStruct((4, r_cols, n_tgt), F32),
            in_specs=[smem, smem] + [vmem] * 5,
            out_specs=vmem,
            scratch_shapes=[pltpu.SMEM((8,), jnp.int32)],
            compiler_params=pltpu.CompilerParams(vmem_limit_bytes=20 * 2**20),
        )(length_scale, out_scale, *gathered)
        y_t = pl.pallas_call(
            sum_kernel,
            out_shape=jax.ShapeDtypeStruct((r_cols, n_tgt), F32),
            in_specs=[smem, smem] + [vmem] * 5,
            out_specs=vmem,
            scratch_shapes=[pltpu.VMEM((3, r_cols, n_tgt), F32), dma((3,)), dma((3,))],
            compiler_params=pltpu.CompilerParams(
                collective_id=1, has_side_effects=True, vmem_limit_bytes=20 * 2**20),
        )(length_scale, out_scale, *gathered[:4], partial)
        return y_t.T

    return jax.shard_map(local_fn, mesh=mesh, in_specs=(row_spec, row_spec, row_spec, row_spec, P(None), P(None)),
                         out_specs=row_spec, check_vma=False)
```
